32 devices in a mesh: expert: 8 (over z, y), gate: 4 (over x, core).
Axes of the slice: x: 2, y: 2, z: 4, core: 2. Of those that a mesh axis runs over, the one named last changes fastest.
Arguments:
- samples: bfloat16 [6144, 4096], P('expert', 'gate'), may hold values from -4 to 4
- gate_weight: bfloat16 [4096, 32], P('gate'), may hold values from -1 to 1
- expert_ids: int32 [6144, 2], P('expert'), may hold values from 0 to 31, all different within a row; in each aligned block of 768 rows (0 to 767, 768 to 1535, ...) at most 96 rows name the same one
- pad_mask: int32 [6144], P('expert'), may hold values 0 or 1
- up_weight: bfloat16 [32, 4096, 1024], P(('expert', 'gate')), may hold values from -0.09375 to 0.09375
- down_weight: bfloat16 [32, 1024, 1024], P(('expert', 'gate')), may hold values from -0.1875 to 0.1875
Outputs:
- combined: bfloat16 [6144, 1024], P('expert', 'gate')
The draws below stay inside these ranges and needn't reach their ends.
Inputs may be any that keep to these rules, and one draw needn't show every extreme that they name: `expert_ids`: each sample names two different experts; among the 768 samples of one index of expert no expert is named more than 96 times, a bound that some block reaches.
All inputs are finite; a program needn't handle non-finite values. No bound on the sum of `pad_mask` on one device may be relied on, other than what follows from the above.
Results may differ from the reference program's by a relative error of at most 0.0057.
Values may be sent and summed in bfloat16 or wider, within the bound.
A program may use at most 128 MiB of HBM per device.

```python
import math
import jax
import jax.numpy as jnp
import numpy as np
from jax import lax

D = 4096
H = 1024
OUT = 1024
ROWS_DEV = 768
EXPERTS = 32
CAP = 96
BATCH = 6144
N_EXPERT = 8


def draw_samples(key, part):
    inner = jax.random.fold_in(key, 3)
    drawn = jnp.clip(jax.random.normal(inner, (BATCH, D), jnp.float32), -4.0, 4.0)
    return drawn.astype(jnp.bfloat16)


def draw_gate_weight(key, part):
    inner = jax.random.fold_in(key, 5)
    spread_key = jax.random.fold_in(key, 6)
    scales = jnp.exp(jax.random.uniform(spread_key, (1, EXPERTS), jnp.float32, jnp.log(0.15), jnp.log(1.5)))
    drawn = jnp.clip(jax.random.normal(inner, (D, EXPERTS), jnp.float32), -4.0, 4.0)
    drawn = drawn * scales / jnp.sqrt(jnp.float32(D))
    return drawn.astype(jnp.bfloat16)


def place_ends(entries, rng, low, high):
    place = [jax.random.randint(jax.random.fold_in(rng, axis), (), 0, length) for axis, length in enumerate(entries.shape)]
    longest = entries.shape.index(max(entries.shape))
    neighbour = place[:longest] + [(place[longest] + 1) % entries.shape[longest]] + place[longest + 1:]
    return entries.at[tuple(place)].set(low).at[tuple(neighbour)].set(high)


def levels(key, extent, cuts, low, largest):
    def one(dim, blocks):
        draws = jax.random.uniform(jax.random.fold_in(jax.random.fold_in(key, 6), dim), (blocks,), jnp.float32, low / len(cuts), largest / len(cuts))
        return jnp.repeat(jnp.exp(draws), extent[dim] // blocks).reshape((-1,) + (1,) * (len(extent) - dim - 1))

    loudness = one(*cuts[0])
    for cut in cuts[1:]:
        loudness = loudness * one(*cut)
    return loudness


def routed_block(rng, own, number, rows, number_of, top, reach, skew):
    order = jax.random.permutation(rng, number_of)
    packed, usual = portions_of(number_of, rows * top, reach, skew, True), portions_of(number_of, rows * top, reach, skew, False)
    places = jnp.arange(number_of)

    def named(sizes, offset_by):
        used = int((sizes > 0).sum())
        fixed = max(1, used // 4)
        moved = fixed + (places - fixed + offset_by * (used - fixed)) % max(1, number_of - fixed)
        return jnp.zeros((number_of,), jnp.int32).at[order[jnp.where(places < fixed, places, moved)]].set(jnp.asarray(sizes, jnp.int32))

    sizes = jnp.where(number % 4 == 0, named(packed, number // 4), named(usual, number - number // 4 - 1))
    mixed = jax.random.permutation(jax.random.fold_in(own, 3), number_of)
    source_of, taker = mixed[0:number_of // 2 * 2:2], mixed[1:number_of // 2 * 2:2]
    room = jnp.minimum(sizes[source_of] - 1, reach - sizes[taker]) // 2
    room = jnp.where((source_of == order[0]) | (taker == order[0]) | (sizes[taker] == 0), 0, jnp.maximum(room, 0))
    moved = jax.random.randint(jax.random.fold_in(own, 4), (number_of // 2,), 0, 1 << 20) % (room + 1)
    sizes = sizes.at[source_of].add(-moved).at[taker].add(moved)
    labels = jnp.searchsorted(jnp.cumsum(sizes), jnp.arange(rows * top), side="right").astype(jnp.int32)
    listing = labels.reshape(top, rows).T
    listing = listing[jax.random.permutation(jax.random.fold_in(own, 1), rows)]
    offset_by = jax.random.randint(jax.random.fold_in(own, 2), (rows, 1), 0, top)
    return jnp.take_along_axis(listing, (jnp.arange(top)[None, :] + offset_by) % top, axis=1)


def portions_of(number_of, total, limit, slope, full):
    weights = [(1 << 20) // math.isqrt(standing ** slope) + 1 for standing in range(1, number_of + 1)]
    largest = limit if full else min(limit, max(-(-total // number_of), total * weights[0] // sum(weights)))
    least = 1 if total - largest >= number_of - 1 else 0
    counts, rest = [largest] + [least] * (number_of - 1), total - largest - least * (number_of - 1)
    while rest > 0:
        movable = [i for i in range(1, number_of) if counts[i] < largest] or [i for i in range(1, number_of) if counts[i] < limit]
        whole, budget = sum([weights[i] for i in movable]), rest
        for i in movable:
            addition = min(limit - counts[i], max(1, budget * weights[i] // whole), rest)
            counts[i] = counts[i] + addition
            rest = rest - addition
    return np.array(counts)


def noise(stream_key, extent, spread, most, cuts=(), kind=jnp.bfloat16):
    gain = levels(stream_key, extent, cuts, -0.22, 0.18) if cuts else 1.0
    drawn = jax.random.normal(stream_key, extent, jnp.float32) * spread * gain
    return jnp.minimum(jnp.maximum(drawn, -most), most).astype(kind)


def setup_inputs(seed: int = 0) -> dict:
    key_of = jax.random.split(jax.random.key(seed), 7)
    samples = draw_samples(jax.random.fold_in(key_of[6], 71), 0)
    gate_weight = draw_gate_weight(jax.random.fold_in(key_of[6], 71), 0)
    expert_ids_keys = jax.random.split(jax.random.fold_in(key_of[2], 1), BATCH // ROWS_DEV)
    expert_ids_turns = jax.random.permutation(jax.random.fold_in(key_of[2], 3), BATCH // ROWS_DEV)
    expert_ids = jax.vmap(lambda own, number: routed_block(jax.random.fold_in(key_of[2], 2), own, number, ROWS_DEV, EXPERTS, 2, CAP, 1))(expert_ids_keys, expert_ids_turns).reshape((BATCH, 2))
    pad_mask = place_ends((jax.random.randint(key_of[3], (BATCH,), 0, 8) < 7).astype(jnp.int32), jax.random.fold_in(key_of[3], 1), 0, 1)
    up_weight = noise(key_of[4], (EXPERTS, D, H), D ** -0.5, 0.09375, ((0, 32),))
    down_weight = noise(key_of[5], (EXPERTS, H, OUT), H ** -0.5, 0.1875, ((0, 32),))
    return {"samples": samples, "gate_weight": gate_weight, "expert_ids": expert_ids, "pad_mask": pad_mask, "up_weight": up_weight, "down_weight": down_weight}


def reference(samples, gate_weight, expert_ids, pad_mask, up_weight, down_weight):
    logits = jnp.dot(samples, gate_weight, preferred_element_type=jnp.float32)
    row_top = jnp.max(logits, axis=1, keepdims=True)
    row_total = jnp.sum(jnp.exp(logits - row_top), axis=1, keepdims=True)
    chosen = jnp.take_along_axis(logits, expert_ids, axis=1)
    factor = EXPERTS * jnp.exp(chosen - row_top) / row_total * pad_mask.astype(jnp.float32)[:, None]
    grouped = expert_ids.reshape(N_EXPERT, ROWS_DEV * 2)
    onehot = (grouped[:, :, None] == jnp.arange(EXPERTS, dtype=jnp.int32)[None, None, :]).astype(jnp.int32)
    slot_rank = jnp.sum(onehot * (jnp.cumsum(onehot, axis=1) - 1), axis=2)
    source_index = jnp.arange(N_EXPERT, dtype=jnp.int32)[:, None]
    position = (grouped * (N_EXPERT * CAP) + source_index * CAP + slot_rank).reshape(-1).astype(jnp.int32)
    row_index = jnp.repeat(jnp.arange(BATCH, dtype=jnp.int32), 2)
    owners = jnp.full((EXPERTS * N_EXPERT * CAP,), BATCH, jnp.int32).at[position].set(row_index)
    padded = jnp.concatenate([samples, jnp.zeros((1, D), samples.dtype)], axis=0)

    def expert_pass(operands):
        owner_block, first, second = operands
        slot_block = padded[owner_block]
        hidden = jnp.dot(slot_block, first, preferred_element_type=jnp.float32)
        active = jnp.maximum(hidden, 0.0).astype(jnp.bfloat16)
        return jnp.dot(active, second, preferred_element_type=jnp.float32).astype(jnp.bfloat16)

    results = lax.map(expert_pass, (owners.reshape(EXPERTS, N_EXPERT * CAP), up_weight, down_weight))
    flat_out = results.reshape(EXPERTS * N_EXPERT * CAP, OUT)
    picked = flat_out[position].astype(jnp.float32).reshape(BATCH, 2, OUT)
    return jnp.sum(factor[:, :, None] * picked, axis=1).astype(jnp.bfloat16)
```

```python
import jax
import jax.numpy as jnp
from jax import lax
from jax.sharding import PartitionSpec as P


def routing(expert_ids, expert_count):
    row_count = expert_ids.shape[0]
    lanes = jnp.arange(expert_count, dtype=jnp.int32)[None, :]
    first = expert_ids[:, 0:1] == lanes
    second = expert_ids[:, 1:2] == lanes
    member = first | second
    rows = jnp.arange(row_count, dtype=jnp.int32)
    lower = (rows[:, None] > rows[None, :]).astype(jnp.bfloat16)
    before = jnp.dot(lower, member.astype(jnp.bfloat16), preferred_element_type=jnp.float32)
    before = before.astype(jnp.int32)
    return first, second, member, before


def factors(logits, first, second, pad_mask, expert_count):
    top = jnp.max(logits, axis=1, keepdims=True)
    terms = jnp.exp(logits - top)
    scale = pad_mask.astype(jnp.float32)[:, None] / jnp.sum(terms, axis=1, keepdims=True)
    factor0 = expert_count * jnp.sum(jnp.where(first, terms, 0.0), axis=1, keepdims=True) * scale
    factor1 = expert_count * jnp.sum(jnp.where(second, terms, 0.0), axis=1, keepdims=True) * scale
    return factor0, factor1


def per_device(samples, gate_weight, expert_ids, pad_mask, up_weight, down_weight):
    row_count, share = samples.shape
    group_count = lax.axis_size("expert")
    gate_count = lax.axis_size("gate")
    expert_count = group_count * gate_count
    capacity = 4 * row_count // expert_count
    partial = jnp.dot(samples, gate_weight, preferred_element_type=jnp.float32)
    logits = jnp.sum(lax.all_gather(partial, "gate"), axis=0)
    first, second, member, before = routing(expert_ids, expert_count)
    place = jnp.where(member, before, -1).T
    ranks = jnp.arange(capacity, dtype=jnp.int32)
    send = (place[:, None, :] == ranks[None, :, None]).astype(jnp.bfloat16)
    outgoing = jnp.dot(
        send.reshape(expert_count * capacity, row_count), samples, preferred_element_type=jnp.float32
    ).astype(jnp.bfloat16)
    incoming = lax.all_to_all(
        outgoing.reshape(expert_count, capacity, share),
        ("expert", "gate"),
        split_axis=0,
        concat_axis=0,
        tiled=True,
    ).reshape(group_count, gate_count, capacity, share)
    hidden = 0.0
    for g in range(gate_count):
        hidden += jnp.dot(
            incoming[:, g].reshape(group_count * capacity, share),
            up_weight[0, g * share : (g + 1) * share],
            preferred_element_type=jnp.float32,
        )
    active = jnp.maximum(hidden, 0.0).astype(jnp.bfloat16)
    expert_out = jnp.dot(active, down_weight[0], preferred_element_type=jnp.float32).astype(
        jnp.bfloat16
    )
    out_share = expert_out.shape[1] // gate_count
    outbound = expert_out.reshape(group_count, capacity, gate_count, out_share)
    outbound = outbound.transpose(0, 2, 1, 3).reshape(expert_count, capacity, out_share)
    returned = lax.all_to_all(
        outbound, ("expert", "gate"), split_axis=0, concat_axis=0, tiled=True
    ).reshape(expert_count * capacity, out_share)
    factor0, factor1 = factors(logits, first, second, pad_mask, expert_count)
    slots = jnp.arange(expert_count * capacity, dtype=jnp.int32)[None, :]
    mixed = 0.0
    for k, (chosen, factor) in enumerate(((first, factor0), (second, factor1))):
        rank = jnp.sum(jnp.where(chosen, before, 0), axis=1, keepdims=True)
        position = expert_ids[:, k : k + 1] * capacity + rank
        pick = (position == slots).astype(jnp.bfloat16)
        mixed += factor * jnp.dot(pick, returned, preferred_element_type=jnp.float32)
    return mixed.astype(jnp.bfloat16)


def solution(mesh):
    placed = (
        P("expert", "gate"),
        P("gate", None),
        P("expert", None),
        P("expert"),
        P(("expert", "gate"), None, None),
        P(("expert", "gate"), None, None),
    )
    return jax.shard_map(
        per_device, mesh=mesh, in_specs=placed, out_specs=P("expert", "gate"), check_vma=False
    )
```

```python
import functools

import jax
import jax.numpy as jnp
from jax import lax
from jax.experimental import pallas as pl
from jax.experimental.pallas import tpu as pltpu
from jax.sharding import PartitionSpec as P


MESH = pl.DeviceIdType.MESH
CHUNKS = 4
SIDES = 2


def routing(expert_ids, expert_count):
    row_count = expert_ids.shape[0]
    lanes = jnp.arange(expert_count, dtype=jnp.int32)[None, :]
    first = expert_ids[:, 0:1] == lanes
    second = expert_ids[:, 1:2] == lanes
    member = first | second
    rows = jnp.arange(row_count, dtype=jnp.int32)
    lower = (rows[:, None] > rows[None, :]).astype(jnp.bfloat16)
    before = jnp.dot(lower, member.astype(jnp.bfloat16), preferred_element_type=jnp.float32)
    before = before.astype(jnp.int32)
    return first, second, member, before


def factors(logits, first, second, pad_mask, expert_count):
    top = jnp.max(logits, axis=1, keepdims=True)
    terms = jnp.exp(logits - top)
    scale = pad_mask.astype(jnp.float32)[:, None] / jnp.sum(terms, axis=1, keepdims=True)
    factor0 = expert_count * jnp.sum(jnp.where(first, terms, 0.0), axis=1, keepdims=True) * scale
    factor1 = expert_count * jnp.sum(jnp.where(second, terms, 0.0), axis=1, keepdims=True) * scale
    return factor0, factor1


def copied(source, target, sem):
    return pltpu.make_async_copy(source, target, sem)


def sent(source, target, send_sem, recv_sem, device):
    return pltpu.make_async_remote_copy(
        src_ref=source,
        dst_ref=target,
        send_sem=send_sem,
        recv_sem=recv_sem,
        device_id=device,
        device_id_type=MESH,
    )


def table(values, index):
    out = values[0]
    for k in range(1, len(values)):
        out = jnp.where(index == k, values[k], out)
    return out


def exchange_kernel(
    planes,
    gates,
    capacity,
    samples,
    place,
    partial,
    up,
    down,
    ret,
    logits,
    blocks,
    places,
    onehot,
    dbuf,
    inc,
    upv,
    downv,
    hidden,
    obuf,
    own_sem,
    w_sem,
    zs_up,
    zs_down,
    zs_relay,
    zr,
    ps,
    pr,
    rs,
    rr,
    ms,
    mr,
    gs,
    gr,
    l_sem,
):
    chunks = CHUNKS
    local = SIDES * gates
    e = lax.axis_index("expert")
    g = lax.axis_index("gate")
    z = e // SIDES
    y = lax.rem(e, SIDES)
    mine = y * gates + g
    me = e * gates + g
    total = planes * local
    rows = blocks.shape[2]
    width = blocks.shape[3]
    slots = local * capacity

    own = [
        copied(samples.at[:, pl.ds(c * width, width)], blocks.at[z, c], own_sem.at[c])
        for c in range(chunks)
    ]
    for copy in own:
        copy.start()
    weights = (copied(up.at[0], upv, w_sem.at[0]), copied(down.at[0], downv, w_sem.at[1]))
    small = (
        copied(place.at[pl.ds(z * local, local)], places.at[z], l_sem.at[0]),
        copied(partial, logits.at[g], l_sem.at[1]),
    )
    for copy in small:
        copy.start()

    barrier = pltpu.get_barrier_semaphore()

    def greet(d, carry):
        t = lax.rem(me + d, total)
        pl.semaphore_signal(
            barrier, inc=1, device_id=(t // gates, lax.rem(t, gates)), device_id_type=MESH
        )
        return carry

    lax.fori_loop(1, total, greet, 0)
    pl.semaphore_wait(barrier, total - 1)

    routes = []
    for d in range(1, planes):
        j = lax.rem(z + d, planes)
        routes.append(
            sent(
                place.at[pl.ds(j * local, local)],
                places.at[z],
                ms.at[d - 1],
                mr.at[z],
                (j * SIDES + y, g),
            )
        )
        routes[-1].start()
    up_ok = z + 1 < planes
    down_ok = z >= 1

    def shift(j, c, sem, step):
        return sent(
            blocks.at[j, c], blocks.at[j, c], sem, zr.at[j, c], ((z + step) * SIDES + y, g)
        )

    for c in range(chunks):
        own[c].wait()

        @pl.when(up_ok)
        def _():
            shift(z, c, zs_up.at[c], 1).start()

        @pl.when(down_ok)
        def _():
            shift(z, c, zs_down.at[c], -1).start()

    for copy in weights:
        copy.start()
    gate_routes = []
    for d in range(1, gates):
        t = lax.rem(g + d, gates)
        gate_routes.append(sent(partial, logits.at[g], gs.at[d - 1], gr.at[d - 1], (e, t)))
        gate_routes[-1].start()
    for copy in small:
        copy.wait()

    orders = [sorted(range(planes), key=lambda j: (abs(j - k), j)) for k in range(planes)]

    def block_at(p):
        return table([table(order, p) for order in orders], z)

    def relay_up(j):
        return (j < z) & up_ok

    def relay_down(j):
        return (j > z) & down_ok

    items = planes * chunks

    def dispatch(t):
        j = block_at(t // chunks)
        c = lax.rem(t, chunks)

        @pl.when(j != z)
        def _():
            copied(blocks.at[j, c], blocks.at[j, c], zr.at[j, c]).wait()

            @pl.when(relay_up(j))
            def _():
                shift(j, c, zs_relay.at[j, c], 1).start()

            @pl.when(relay_down(j))
            def _():
                shift(j, c, zs_relay.at[j, c], -1).start()

        @pl.when(c == 0)
        def _():
            @pl.when(j != z)
            def _():
                copied(places.at[j], places.at[j], mr.at[j]).wait()

            ranks = lax.broadcasted_iota(jnp.int32, (capacity, rows), 0).astype(jnp.float32)
            for i in range(local):
                line = places[j, i : i + 1, :]
                onehot[i * capacity : (i + 1) * capacity, :] = jnp.where(
                    line == ranks, 1.0, 0.0
                ).astype(jnp.bfloat16)

        half = slots // 2
        for h in range(2):
            picked = jnp.dot(
                onehot[h * half : (h + 1) * half, :],
                blocks[j, c],
                preferred_element_type=jnp.float32,
            ).astype(jnp.bfloat16)
            dbuf[j, c, h * half : (h + 1) * half, :] = picked

        def give(d, carry):
            i = lax.rem(mine + d, local)
            sent(
                dbuf.at[j, c, pl.ds(i * capacity, capacity)],
                inc.at[j, c, g, pl.ds(y * capacity, capacity)],
                ps,
                pr.at[j, c],
                (z * SIDES + i // gates, lax.rem(i, gates)),
            ).start()
            return carry

        lax.fori_loop(1, local, give, 0)
        copied(
            dbuf.at[j, c, pl.ds(mine * capacity, capacity)],
            inc.at[j, c, g, pl.ds(y * capacity, capacity)],
            pr.at[j, c],
        ).start()

    def expert(t):
        j = block_at(t // chunks)
        c = lax.rem(t, chunks)
        copied(inc.at[j, c], inc.at[j, c], pr.at[j, c]).wait()
        share = width * chunks
        tile = 256
        for n in range(hidden.shape[1] // tile):
            cols = slice(n * tile, (n + 1) * tile)
            acc = jnp.zeros((SIDES * capacity, tile), jnp.float32)
            for k in range(gates):
                start = pl.multiple_of(k * share + c * width, width)
                acc += jnp.dot(
                    inc[j, c, k], upv[pl.ds(start, width), cols], preferred_element_type=jnp.float32
                )

            @pl.when(c == 0)
            def _():
                hidden[:, cols] = acc

            @pl.when(c != 0)
            def _():
                hidden[:, cols] += acc

        @pl.when(c == chunks - 1)
        def _():
            active = jnp.maximum(hidden[...], 0.0).astype(jnp.bfloat16)
            out_width = downv.shape[1] // gates
            for k in range(gates):
                out = jnp.dot(
                    active,
                    downv[:, k * out_width : (k + 1) * out_width],
                    preferred_element_type=jnp.float32,
                ).astype(jnp.bfloat16)
                obuf[j, k] = out

            def hand(i, carry):
                side, k = i // gates, lax.rem(i, gates)
                block = obuf.at[j, k, pl.ds(side * capacity, capacity)]
                away = (j != z) | (i != mine)

                @pl.when(away)
                def _():
                    sent(block, ret.at[me], rs, rr.at[me], (j * SIDES + side, k)).start()

                @pl.when(jnp.logical_not(away))
                def _():
                    copied(block, ret.at[me], rr.at[me]).start()

                return carry

            lax.fori_loop(0, local, hand, 0)

    def step(t, carry):
        @pl.when(t < items)
        def _():
            dispatch(t)

        @pl.when(t == 1)
        def _():
            for copy in weights:
                copy.wait()

        @pl.when(t >= 1)
        def _():
            expert(t - 1)

        return carry

    lax.fori_loop(0, items + 1, step, 0)

    for copy in routes + gate_routes:
        copy.wait_send()
    for copy in gate_routes:
        copy.wait_recv()
    for c in range(chunks):

        @pl.when(up_ok)
        def _():
            shift(z, c, zs_up.at[c], 1).wait_send()

        @pl.when(down_ok)
        def _():
            shift(z, c, zs_down.at[c], -1).wait_send()

    def relayed(t, carry):
        j, c = t // chunks, lax.rem(t, chunks)

        @pl.when(relay_up(j) | relay_down(j))
        def _():
            copied(blocks.at[j, c], blocks.at[j, c], zs_relay.at[j, c]).wait()

        return carry

    lax.fori_loop(0, items, relayed, 0)
    given = dbuf.at[:, :, pl.ds(0, slots - capacity)]
    copied(given, given, ps).wait()
    handed = ret.at[pl.ds(0, total - 1)]
    copied(handed, handed, rs).wait()

    def arrived(i, carry):
        copied(ret.at[i], ret.at[i], rr.at[i]).wait()
        return carry

    lax.fori_loop(0, total, arrived, 0)


def exchange(samples, place, partial, up, down, planes, gates, capacity):
    rows, share = samples.shape
    local = SIDES * gates
    total = planes * local
    width = share // CHUNKS
    depth, inner = up.shape[1:]
    outer = down.shape[2]
    out_width = outer // gates
    bf16, f32 = jnp.bfloat16, jnp.float32
    dma = pltpu.SemaphoreType.DMA
    vmem = pl.BlockSpec(memory_space=pltpu.VMEM)
    hbm = pl.BlockSpec(memory_space=pl.ANY)
    return pl.pallas_call(
        functools.partial(exchange_kernel, planes, gates, capacity),
        out_shape=(
            jax.ShapeDtypeStruct((total, capacity, out_width), bf16),
            jax.ShapeDtypeStruct((gates,) + partial.shape, f32),
        ),
        in_specs=[hbm, vmem, vmem, hbm, hbm],
        out_specs=(vmem, vmem),
        scratch_shapes=[
            pltpu.VMEM((planes, CHUNKS, rows, width), bf16),
            pltpu.VMEM((planes, local, rows), f32),
            pltpu.VMEM((local * capacity, rows), bf16),
            pltpu.VMEM((planes, CHUNKS, local * capacity, width), bf16),
            pltpu.VMEM((planes, CHUNKS, gates, SIDES * capacity, width), bf16),
            pltpu.VMEM((depth, inner), bf16),
            pltpu.VMEM((inner, outer), bf16),
            pltpu.VMEM((SIDES * capacity, inner), f32),
            pltpu.VMEM((planes, gates, SIDES * capacity, out_width), bf16),
            dma((CHUNKS,)),
            dma((2,)),
            dma((CHUNKS,)),
            dma((CHUNKS,)),
            dma((planes, CHUNKS)),
            dma((planes, CHUNKS)),
            dma,
            dma((planes, CHUNKS)),
            dma,
            dma((total,)),
            dma((planes,)),
            dma((planes,)),
            dma((gates,)),
            dma((gates,)),
            dma((2,)),
        ],
        compiler_params=pltpu.CompilerParams(
            collective_id=0, has_side_effects=True, vmem_limit_bytes=56 << 20
        ),
    )(samples, place, partial, up, down)


def combine(returned, expert_ids, first, second, before, factor0, factor1, capacity):
    slots = jnp.arange(returned.shape[0], dtype=jnp.int32)[None, :]
    mixed = 0.0
    for k, (chosen, factor) in enumerate(((first, factor0), (second, factor1))):
        rank = jnp.sum(jnp.where(chosen, before, 0), axis=1, keepdims=True)
        position = expert_ids[:, k : k + 1] * capacity + rank
        pick = (position == slots).astype(jnp.bfloat16)
        mixed += factor * jnp.dot(pick, returned, preferred_element_type=jnp.float32)
    return mixed.astype(jnp.bfloat16)


def in_one_kernel(samples, gate_weight, expert_ids, pad_mask, up_weight, down_weight):
    group_count = lax.axis_size("expert")
    gate_count = lax.axis_size("gate")
    expert_count = group_count * gate_count
    capacity = 4 * samples.shape[0] // expert_count
    partial = lax.dot_general(
        gate_weight, samples, (((0,), (1,)), ((), ())), preferred_element_type=jnp.float32
    )
    first, second, member, before = routing(expert_ids, expert_count)
    place = jnp.where(member, before, -1).T.astype(jnp.float32)
    returned, logits = exchange(
        samples, place, partial, up_weight, down_weight, group_count // SIDES, gate_count, capacity
    )
    returned = returned.reshape(expert_count * capacity, -1)
    logits = jnp.sum(logits, axis=0).T
    factor0, factor1 = factors(logits, first, second, pad_mask, expert_count)
    return combine(returned, expert_ids, first, second, before, factor0, factor1, capacity)


def fits(samples, up_weight, down_weight):
    group_count = lax.axis_size("expert")
    capacity = 4 * samples.shape[0] // (group_count * lax.axis_size("gate"))
    planes = group_count // SIDES
    held = 2 * (planes * samples.size * 3 + up_weight.size + down_weight.size)
    return group_count % SIDES == 0 and capacity % 16 == 0 and held < 40 << 20


def per_device(samples, gate_weight, expert_ids, pad_mask, up_weight, down_weight):
    if fits(samples, up_weight, down_weight):
        return in_one_kernel(
            samples, gate_weight, expert_ids, pad_mask, up_weight, down_weight
        )
    row_count, share = samples.shape
    group_count = lax.axis_size("expert")
    gate_count = lax.axis_size("gate")
    expert_count = group_count * gate_count
    capacity = 4 * row_count // expert_count
    partial = jnp.dot(samples, gate_weight, preferred_element_type=jnp.float32)
    logits = jnp.sum(lax.all_gather(partial, "gate"), axis=0)
    first, second, member, before = routing(expert_ids, expert_count)
    place = jnp.where(member, before, -1).T
    ranks = jnp.arange(capacity, dtype=jnp.int32)
    send = (place[:, None, :] == ranks[None, :, None]).astype(jnp.bfloat16)
    outgoing = jnp.dot(
        send.reshape(expert_count * capacity, row_count), samples, preferred_element_type=jnp.float32
    ).astype(jnp.bfloat16)
    incoming = lax.all_to_all(
        outgoing.reshape(expert_count, capacity, share),
        ("expert", "gate"),
        split_axis=0,
        concat_axis=0,
        tiled=True,
    ).reshape(group_count, gate_count, capacity, share)
    hidden = 0.0
    for g in range(gate_count):
        hidden += jnp.dot(
            incoming[:, g].reshape(group_count * capacity, share),
            up_weight[0, g * share : (g + 1) * share],
            preferred_element_type=jnp.float32,
        )
    active = jnp.maximum(hidden, 0.0).astype(jnp.bfloat16)
    expert_out = jnp.dot(active, down_weight[0], preferred_element_type=jnp.float32).astype(
        jnp.bfloat16
    )
    out_share = expert_out.shape[1] // gate_count
    outbound = expert_out.reshape(group_count, capacity, gate_count, out_share)
    outbound = outbound.transpose(0, 2, 1, 3).reshape(expert_count, capacity, out_share)
    returned = lax.all_to_all(
        outbound, ("expert", "gate"), split_axis=0, concat_axis=0, tiled=True
    ).reshape(expert_count * capacity, out_share)
    factor0, factor1 = factors(logits, first, second, pad_mask, expert_count)
    slots = jnp.arange(expert_count * capacity, dtype=jnp.int32)[None, :]
    mixed = 0.0
    for k, (chosen, factor) in enumerate(((first, factor0), (second, factor1))):
        rank = jnp.sum(jnp.where(chosen, before, 0), axis=1, keepdims=True)
        position = expert_ids[:, k : k + 1] * capacity + rank
        pick = (position == slots).astype(jnp.bfloat16)
        mixed += factor * jnp.dot(pick, returned, preferred_element_type=jnp.float32)
    return mixed.astype(jnp.bfloat16)


def solution(mesh):
    placed = (
        P("expert", "gate"),
        P("gate", None),
        P("expert", None),
        P("expert"),
        P(("expert", "gate"), None, None),
        P(("expert", "gate"), None, None),
    )
    return jax.shard_map(
        per_device, mesh=mesh, in_specs=placed, out_specs=P("expert", "gate"), check_vma=False
    )
```

```python
import functools

import jax
import jax.numpy as jnp
from jax import lax
from jax.experimental import pallas as pl
from jax.experimental.pallas import tpu as pltpu
from jax.sharding import PartitionSpec as P


MESH = pl.DeviceIdType.MESH
CHUNKS = 4
SIDES = 2


def routing(expert_ids, expert_count):
    row_count = expert_ids.shape[0]
    lanes = jnp.arange(expert_count, dtype=jnp.int32)[None, :]
    first = expert_ids[:, 0:1] == lanes
    second = expert_ids[:, 1:2] == lanes
    member = first | second
    rows = jnp.arange(row_count, dtype=jnp.int32)
    lower = (rows[:, None] > rows[None, :]).astype(jnp.bfloat16)
    before = jnp.dot(lower, member.astype(jnp.bfloat16), preferred_element_type=jnp.float32)
    before = before.astype(jnp.int32)
    return first, second, member, before


def factors(logits, first, second, pad_mask, expert_count):
    top = jnp.max(logits, axis=1, keepdims=True)
    terms = jnp.exp(logits - top)
    scale = pad_mask.astype(jnp.float32)[:, None] / jnp.sum(terms, axis=1, keepdims=True)
    factor0 = expert_count * jnp.sum(jnp.where(first, terms, 0.0), axis=1, keepdims=True) * scale
    factor1 = expert_count * jnp.sum(jnp.where(second, terms, 0.0), axis=1, keepdims=True) * scale
    return factor0, factor1


def copied(source, target, sem):
    return pltpu.make_async_copy(source, target, sem)


def sent(source, target, send_sem, recv_sem, device):
    return pltpu.make_async_remote_copy(
        src_ref=source,
        dst_ref=target,
        send_sem=send_sem,
        recv_sem=recv_sem,
        device_id=device,
        device_id_type=MESH,
    )


def table(values, index):
    out = values[0]
    for k in range(1, len(values)):
        out = jnp.where(index == k, values[k], out)
    return out


def exchange_kernel(
    planes,
    gates,
    capacity,
    samples,
    place,
    gate_weight,
    up,
    down,
    ret,
    logits,
    blocks,
    places,
    onehot,
    dbuf,
    inc,
    upv,
    downv,
    hidden,
    obuf,
    own_sem,
    w_sem,
    zs_up,
    zs_down,
    zs_relay,
    zr,
    ps,
    pr,
    rs,
    rr,
    ms,
    mr,
    gs,
    gr,
    l_sem,
):
    chunks = CHUNKS
    local = SIDES * gates
    e = lax.axis_index("expert")
    g = lax.axis_index("gate")
    z = e // SIDES
    y = lax.rem(e, SIDES)
    mine = y * gates + g
    me = e * gates + g
    total = planes * local
    rows = blocks.shape[2]
    width = blocks.shape[3]
    slots = local * capacity

    own = [
        copied(samples.at[:, pl.ds(c * width, width)], blocks.at[z, c], own_sem.at[c])
        for c in range(chunks)
    ]
    for copy in own:
        copy.start()
    weights = (copied(up.at[0], upv, w_sem.at[0]), copied(down.at[0], downv, w_sem.at[1]))
    kept = copied(place.at[pl.ds(z * local, local)], places.at[z], l_sem)
    kept.start()

    barrier = pltpu.get_barrier_semaphore()

    def greet(d, carry):
        t = lax.rem(me + d, total)
        pl.semaphore_signal(
            barrier, inc=1, device_id=(t // gates, lax.rem(t, gates)), device_id_type=MESH
        )
        return carry

    lax.fori_loop(1, total, greet, 0)
    pl.semaphore_wait(barrier, total - 1)

    routes = []
    for d in range(1, planes):
        j = lax.rem(z + d, planes)
        routes.append(
            sent(
                place.at[pl.ds(j * local, local)],
                places.at[z],
                ms.at[d - 1],
                mr.at[z],
                (j * SIDES + y, g),
            )
        )
        routes[-1].start()
    up_ok = z + 1 < planes
    down_ok = z >= 1

    def shift(j, c, sem, step):
        return sent(
            blocks.at[j, c], blocks.at[j, c], sem, zr.at[j, c], ((z + step) * SIDES + y, g)
        )

    for c in range(chunks):
        own[c].wait()

        @pl.when(up_ok)
        def _():
            shift(z, c, zs_up.at[c], 1).start()

        @pl.when(down_ok)
        def _():
            shift(z, c, zs_down.at[c], -1).start()

    for copy in weights:
        copy.start()
    partial = 0.0
    for c in range(chunks):
        partial += lax.dot_general(
            gate_weight[:, c * width : (c + 1) * width],
            blocks[z, c],
            (((1,), (1,)), ((), ())),
            preferred_element_type=jnp.float32,
        )
    logits[g] = partial
    kept.wait()
    gate_routes = []
    for d in range(1, gates):
        t = lax.rem(g + d, gates)
        gate_routes.append(sent(logits.at[g], logits.at[g], gs.at[d - 1], gr.at[d - 1], (e, t)))

    orders = [sorted(range(planes), key=lambda j: (abs(j - k), j)) for k in range(planes)]

    def block_at(p):
        return table([table(order, p) for order in orders], z)

    def relay_up(j):
        return (j < z) & up_ok

    def relay_down(j):
        return (j > z) & down_ok

    items = planes * chunks

    def held_back(j):
        return up_ok & down_ok & ((j == 0) | (j == planes - 1))

    def give_back(j):
        def hand(i, carry):
            side, k = i // gates, lax.rem(i, gates)
            block = obuf.at[j, k, pl.ds(side * capacity, capacity)]
            away = (j != z) | (i != mine)

            @pl.when(away)
            def _():
                sent(block, ret.at[me], rs, rr.at[me], (j * SIDES + side, k)).start()

            @pl.when(jnp.logical_not(away))
            def _():
                copied(block, ret.at[me], rr.at[me]).start()

            return carry

        lax.fori_loop(0, local, hand, 0)

    def dispatch(t):
        j = block_at(t // chunks)
        c = lax.rem(t, chunks)

        @pl.when(j != z)
        def _():
            copied(blocks.at[j, c], blocks.at[j, c], zr.at[j, c]).wait()

            @pl.when(relay_up(j))
            def _():
                shift(j, c, zs_relay.at[j, c], 1).start()

            @pl.when(relay_down(j))
            def _():
                shift(j, c, zs_relay.at[j, c], -1).start()

        @pl.when(c == 0)
        def _():
            @pl.when(j != z)
            def _():
                copied(places.at[j], places.at[j], mr.at[j]).wait()

            ranks = lax.broadcasted_iota(jnp.int32, (capacity, rows), 0).astype(jnp.float32)
            for i in range(local):
                line = places[j, i : i + 1, :]
                onehot[i * capacity : (i + 1) * capacity, :] = jnp.where(
                    line == ranks, 1.0, 0.0
                ).astype(jnp.bfloat16)

        half = slots // 2
        for h in range(2):
            picked = jnp.dot(
                onehot[h * half : (h + 1) * half, :],
                blocks[j, c],
                preferred_element_type=jnp.float32,
            ).astype(jnp.bfloat16)
            dbuf[j, c, h * half : (h + 1) * half, :] = picked

        def give(d, carry):
            i = lax.rem(mine + d, local)
            sent(
                dbuf.at[j, c, pl.ds(i * capacity, capacity)],
                inc.at[j, c, g, pl.ds(y * capacity, capacity)],
                ps,
                pr.at[j, c],
                (z * SIDES + i // gates, lax.rem(i, gates)),
            ).start()
            return carry

        lax.fori_loop(1, local, give, 0)
        copied(
            dbuf.at[j, c, pl.ds(mine * capacity, capacity)],
            inc.at[j, c, g, pl.ds(y * capacity, capacity)],
            pr.at[j, c],
        ).start()

    def expert(t):
        j = block_at(t // chunks)
        c = lax.rem(t, chunks)
        copied(inc.at[j, c], inc.at[j, c], pr.at[j, c]).wait()
        share = width * chunks
        tile = 256
        for n in range(hidden.shape[1] // tile):
            cols = slice(n * tile, (n + 1) * tile)
            acc = jnp.zeros((SIDES * capacity, tile), jnp.float32)
            for k in range(gates):
                start = pl.multiple_of(k * share + c * width, width)
                acc += jnp.dot(
                    inc[j, c, k], upv[pl.ds(start, width), cols], preferred_element_type=jnp.float32
                )

            @pl.when(c == 0)
            def _():
                hidden[:, cols] = acc

            @pl.when(c != 0)
            def _():
                hidden[:, cols] += acc

        @pl.when(c == chunks - 1)
        def _():
            active = jnp.maximum(hidden[...], 0.0).astype(jnp.bfloat16)
            out_width = downv.shape[1] // gates
            for k in range(gates):
                out = jnp.dot(
                    active,
                    downv[:, k * out_width : (k + 1) * out_width],
                    preferred_element_type=jnp.float32,
                ).astype(jnp.bfloat16)
                obuf[j, k] = out

            @pl.when(jnp.logical_not(held_back(j)))
            def _():
                give_back(j)

    def step(t, carry):
        @pl.when(t < items)
        def _():
            dispatch(t)

        @pl.when(t == 1)
        def _():
            for copy in gate_routes:
                copy.start()
            for copy in weights:
                copy.wait()

        @pl.when(t >= 1)
        def _():
            expert(t - 1)

        return carry

    lax.fori_loop(0, items + 1, step, 0)

    for c in range(chunks):

        @pl.when(up_ok)
        def _():
            shift(z, c, zs_up.at[c], 1).wait_send()

        @pl.when(down_ok)
        def _():
            shift(z, c, zs_down.at[c], -1).wait_send()

    def relayed(t, carry):
        j, c = t // chunks, lax.rem(t, chunks)

        @pl.when(relay_up(j) | relay_down(j))
        def _():
            copied(blocks.at[j, c], blocks.at[j, c], zs_relay.at[j, c]).wait()

        return carry

    lax.fori_loop(0, items, relayed, 0)

    @pl.when(up_ok & down_ok)
    def _():
        for j in (0, planes - 1):
            give_back(j)

    for copy in routes + gate_routes:
        copy.wait_send()
    for copy in gate_routes:
        copy.wait_recv()
    given = dbuf.at[:, :, pl.ds(0, slots - capacity)]
    copied(given, given, ps).wait()
    handed = ret.at[pl.ds(0, total - 1)]
    copied(handed, handed, rs).wait()

    def arrived(i, carry):
        copied(ret.at[i], ret.at[i], rr.at[i]).wait()
        return carry

    lax.fori_loop(0, total, arrived, 0)


def exchange(samples, place, gate_weight, up, down, planes, gates, capacity):
    rows, share = samples.shape
    local = SIDES * gates
    total = planes * local
    width = share // CHUNKS
    depth, inner = up.shape[1:]
    outer = down.shape[2]
    out_width = outer // gates
    bf16, f32 = jnp.bfloat16, jnp.float32
    dma = pltpu.SemaphoreType.DMA
    vmem = pl.BlockSpec(memory_space=pltpu.VMEM)
    hbm = pl.BlockSpec(memory_space=pl.ANY)
    return pl.pallas_call(
        functools.partial(exchange_kernel, planes, gates, capacity),
        out_shape=(
            jax.ShapeDtypeStruct((total, capacity, out_width), bf16),
            jax.ShapeDtypeStruct((gates, total, rows), f32),
        ),
        in_specs=[hbm, vmem, vmem, hbm, hbm],
        out_specs=(vmem, vmem),
        scratch_shapes=[
            pltpu.VMEM((planes, CHUNKS, rows, width), bf16),
            pltpu.VMEM((planes, local, rows), f32),
            pltpu.VMEM((local * capacity, rows), bf16),
            pltpu.VMEM((planes, CHUNKS, local * capacity, width), bf16),
            pltpu.VMEM((planes, CHUNKS, gates, SIDES * capacity, width), bf16),
            pltpu.VMEM((depth, inner), bf16),
            pltpu.VMEM((inner, outer), bf16),
            pltpu.VMEM((SIDES * capacity, inner), f32),
            pltpu.VMEM((planes, gates, SIDES * capacity, out_width), bf16),
            dma((CHUNKS,)),
            dma((2,)),
            dma((CHUNKS,)),
            dma((CHUNKS,)),
            dma((planes, CHUNKS)),
            dma((planes, CHUNKS)),
            dma,
            dma((planes, CHUNKS)),
            dma,
            dma((total,)),
            dma((planes,)),
            dma((planes,)),
            dma((gates,)),
            dma((gates,)),
            dma,
        ],
        compiler_params=pltpu.CompilerParams(
            collective_id=0, has_side_effects=True, vmem_limit_bytes=56 << 20
        ),
    )(samples, place, gate_weight, up, down)


def combine(returned, expert_ids, first, second, before, factor0, factor1, capacity):
    slots = jnp.arange(returned.shape[0], dtype=jnp.int32)[None, :]
    mixed = 0.0
    for k, (chosen, factor) in enumerate(((first, factor0), (second, factor1))):
        rank = jnp.sum(jnp.where(chosen, before, 0), axis=1, keepdims=True)
        position = expert_ids[:, k : k + 1] * capacity + rank
        pick = (position == slots).astype(jnp.bfloat16)
        mixed += factor * jnp.dot(pick, returned, preferred_element_type=jnp.float32)
    return mixed.astype(jnp.bfloat16)


def in_one_kernel(samples, gate_weight, expert_ids, pad_mask, up_weight, down_weight):
    group_count = lax.axis_size("expert")
    gate_count = lax.axis_size("gate")
    expert_count = group_count * gate_count
    capacity = 4 * samples.shape[0] // expert_count
    first, second, member, before = routing(expert_ids, expert_count)
    place = jnp.where(member, before, -1).T.astype(jnp.float32)
    returned, logits = exchange(
        samples,
        place,
        gate_weight.T,
        up_weight,
        down_weight,
        group_count // SIDES,
        gate_count,
        capacity,
    )
    returned = returned.reshape(expert_count * capacity, -1)
    logits = jnp.sum(logits, axis=0).T
    factor0, factor1 = factors(logits, first, second, pad_mask, expert_count)
    return combine(returned, expert_ids, first, second, before, factor0, factor1, capacity)


def fits(samples, up_weight, down_weight):
    group_count = lax.axis_size("expert")
    capacity = 4 * samples.shape[0] // (group_count * lax.axis_size("gate"))
    planes = group_count // SIDES
    held = 2 * (planes * samples.size * 3 + up_weight.size + down_weight.size)
    return group_count % SIDES == 0 and capacity % 16 == 0 and held < 40 << 20


def per_device(samples, gate_weight, expert_ids, pad_mask, up_weight, down_weight):
    if fits(samples, up_weight, down_weight):
        return in_one_kernel(
            samples, gate_weight, expert_ids, pad_mask, up_weight, down_weight
        )
    row_count, share = samples.shape
    group_count = lax.axis_size("expert")
    gate_count = lax.axis_size("gate")
    expert_count = group_count * gate_count
    capacity = 4 * row_count // expert_count
    partial = jnp.dot(samples, gate_weight, preferred_element_type=jnp.float32)
    logits = jnp.sum(lax.all_gather(partial, "gate"), axis=0)
    first, second, member, before = routing(expert_ids, expert_count)
    place = jnp.where(member, before, -1).T
    ranks = jnp.arange(capacity, dtype=jnp.int32)
    send = (place[:, None, :] == ranks[None, :, None]).astype(jnp.bfloat16)
    outgoing = jnp.dot(
        send.reshape(expert_count * capacity, row_count), samples, preferred_element_type=jnp.float32
    ).astype(jnp.bfloat16)
    incoming = lax.all_to_all(
        outgoing.reshape(expert_count, capacity, share),
        ("expert", "gate"),
        split_axis=0,
        concat_axis=0,
        tiled=True,
    ).reshape(group_count, gate_count, capacity, share)
    hidden = 0.0
    for g in range(gate_count):
        hidden += jnp.dot(
            incoming[:, g].reshape(group_count * capacity, share),
            up_weight[0, g * share : (g + 1) * share],
            preferred_element_type=jnp.float32,
        )
    active = jnp.maximum(hidden, 0.0).astype(jnp.bfloat16)
    expert_out = jnp.dot(active, down_weight[0], preferred_element_type=jnp.float32).astype(
        jnp.bfloat16
    )
    out_share = expert_out.shape[1] // gate_count
    outbound = expert_out.reshape(group_count, capacity, gate_count, out_share)
    outbound = outbound.transpose(0, 2, 1, 3).reshape(expert_count, capacity, out_share)
    returned = lax.all_to_all(
        outbound, ("expert", "gate"), split_axis=0, concat_axis=0, tiled=True
    ).reshape(expert_count * capacity, out_share)
    factor0, factor1 = factors(logits, first, second, pad_mask, expert_count)
    slots = jnp.arange(expert_count * capacity, dtype=jnp.int32)[None, :]
    mixed = 0.0
    for k, (chosen, factor) in enumerate(((first, factor0), (second, factor1))):
        rank = jnp.sum(jnp.where(chosen, before, 0), axis=1, keepdims=True)
        position = expert_ids[:, k : k + 1] * capacity + rank
        pick = (position == slots).astype(jnp.bfloat16)
        mixed += factor * jnp.dot(pick, returned, preferred_element_type=jnp.float32)
    return mixed.astype(jnp.bfloat16)


def solution(mesh):
    placed = (
        P("expert", "gate"),
        P("gate", None),
        P("expert", None),
        P("expert"),
        P(("expert", "gate"), None, None),
        P(("expert", "gate"), None, None),
    )
    return jax.shard_map(
        per_device, mesh=mesh, in_specs=placed, out_specs=P("expert", "gate"), check_vma=False
    )
```

```python
import functools

import jax
import jax.numpy as jnp
from jax import lax
from jax.experimental import pallas as pl
from jax.experimental.pallas import tpu as pltpu
from jax.sharding import PartitionSpec as P


MESH = pl.DeviceIdType.MESH
CHUNKS = 4
SIDES = 2


def routing(expert_ids, expert_count):
    row_count = expert_ids.shape[0]
    lanes = jnp.arange(expert_count, dtype=jnp.int32)[None, :]
    first = expert_ids[:, 0:1] == lanes
    second = expert_ids[:, 1:2] == lanes
    member = first | second
    rows = jnp.arange(row_count, dtype=jnp.int32)
    lower = (rows[:, None] > rows[None, :]).astype(jnp.bfloat16)
    before = jnp.dot(lower, member.astype(jnp.bfloat16), preferred_element_type=jnp.float32)
    before = before.astype(jnp.int32)
    return first, second, member, before


def factors(logits, first, second, pad_mask, expert_count):
    top = jnp.max(logits, axis=1, keepdims=True)
    terms = jnp.exp(logits - top)
    scale = pad_mask.astype(jnp.float32)[:, None] / jnp.sum(terms, axis=1, keepdims=True)
    factor0 = expert_count * jnp.sum(jnp.where(first, terms, 0.0), axis=1, keepdims=True) * scale
    factor1 = expert_count * jnp.sum(jnp.where(second, terms, 0.0), axis=1, keepdims=True) * scale
    return factor0, factor1


def copied(source, target, sem):
    return pltpu.make_async_copy(source, target, sem)


def sent(source, target, send_sem, recv_sem, device):
    return pltpu.make_async_remote_copy(
        src_ref=source,
        dst_ref=target,
        send_sem=send_sem,
        recv_sem=recv_sem,
        device_id=device,
        device_id_type=MESH,
    )


def table(values, index):
    out = values[0]
    for k in range(1, len(values)):
        out = jnp.where(index == k, values[k], out)
    return out


def exchange_kernel(
    planes,
    gates,
    capacity,
    samples,
    place,
    gate_weight,
    up,
    down,
    ret,
    logits,
    blocks,
    places,
    onehot,
    dbuf,
    inc,
    upv,
    downv,
    hidden,
    obuf,
    own_sem,
    w_sem,
    zs_up,
    zs_down,
    zs_relay,
    zr,
    ps,
    pr,
    rs,
    rr,
    ms,
    mr,
    gs,
    gr,
    l_sem,
):
    chunks = CHUNKS
    local = SIDES * gates
    e = lax.axis_index("expert")
    g = lax.axis_index("gate")
    z = e // SIDES
    y = lax.rem(e, SIDES)
    mine = y * gates + g
    me = e * gates + g
    total = planes * local
    rows = blocks.shape[2]
    width = blocks.shape[3]
    slots = local * capacity

    own = [
        copied(samples.at[:, pl.ds(c * width, width)], blocks.at[z, c], own_sem.at[c])
        for c in range(chunks)
    ]
    for copy in own:
        copy.start()
    weights = (copied(up.at[0], upv, w_sem.at[0]), copied(down.at[0], downv, w_sem.at[1]))
    kept = copied(place.at[pl.ds(z * local, local)], places.at[z], l_sem)
    kept.start()

    barrier = pltpu.get_barrier_semaphore()

    def greet(d, carry):
        t = lax.rem(me + d, total)
        pl.semaphore_signal(
            barrier, inc=1, device_id=(t // gates, lax.rem(t, gates)), device_id_type=MESH
        )
        return carry

    lax.fori_loop(1, total, greet, 0)
    pl.semaphore_wait(barrier, total - 1)

    routes = []
    for d in range(1, planes):
        j = lax.rem(z + d, planes)
        routes.append(
            sent(
                place.at[pl.ds(j * local, local)],
                places.at[z],
                ms.at[d - 1],
                mr.at[z],
                (j * SIDES + y, g),
            )
        )
        routes[-1].start()
    up_ok = z + 1 < planes
    down_ok = z >= 1

    def shift(j, c, sem, step):
        return sent(
            blocks.at[j, c], blocks.at[j, c], sem, zr.at[j, c], ((z + step) * SIDES + y, g)
        )

    for c in range(chunks):
        own[c].wait()

        @pl.when(up_ok)
        def _():
            shift(z, c, zs_up.at[c], 1).start()

        @pl.when(down_ok)
        def _():
            shift(z, c, zs_down.at[c], -1).start()

    for copy in weights:
        copy.start()
    partial = 0.0
    for c in range(chunks):
        partial += lax.dot_general(
            gate_weight[:, c * width : (c + 1) * width],
            blocks[z, c],
            (((1,), (1,)), ((), ())),
            preferred_element_type=jnp.float32,
        )
    logits[g] = partial
    kept.wait()
    gate_routes = []
    for d in range(1, gates):
        t = lax.rem(g + d, gates)
        gate_routes.append(sent(logits.at[g], logits.at[g], gs.at[d - 1], gr.at[d - 1], (e, t)))

    orders = [sorted(range(planes), key=lambda j: (abs(j - k), j)) for k in range(planes)]

    def block_at(p):
        return table([table(order, p) for order in orders], z)

    def relay_up(j):
        return (j < z) & up_ok

    def relay_down(j):
        return (j > z) & down_ok

    items = planes * chunks

    def held_back(j):
        return up_ok & down_ok & ((j == 0) | (j == planes - 1))

    def give_back(j):
        def hand(i, carry):
            side, k = i // gates, lax.rem(i, gates)
            block = obuf.at[j, k, pl.ds(side * capacity, capacity)]
            away = (j != z) | (i != mine)

            @pl.when(away)
            def _():
                sent(block, ret.at[me], rs, rr.at[me], (j * SIDES + side, k)).start()

            @pl.when(jnp.logical_not(away))
            def _():
                copied(block, ret.at[me], rr.at[me]).start()

            return carry

        lax.fori_loop(0, local, hand, 0)

    def item(t):
        u = t - chunks
        in_turn = up_ok & down_ok & (u >= 0) & (u < 2 * chunks)
        p = jnp.where(in_turn, 1 + lax.rem(u + 2 * chunks, 2), t // chunks)
        return p, jnp.where(in_turn, u // 2, lax.rem(t, chunks))

    def dispatch(t):
        p, c = item(t)
        j = block_at(p)
        lane = lax.rem(p, 2)

        @pl.when(j != z)
        def _():
            copied(blocks.at[j, c], blocks.at[j, c], zr.at[j, c]).wait()

            @pl.when(relay_up(j))
            def _():
                shift(j, c, zs_relay.at[j, c], 1).start()

            @pl.when(relay_down(j))
            def _():
                shift(j, c, zs_relay.at[j, c], -1).start()

        @pl.when(c == 0)
        def _():
            @pl.when(j != z)
            def _():
                copied(places.at[j], places.at[j], mr.at[j]).wait()

            ranks = lax.broadcasted_iota(jnp.int32, (capacity, rows), 0).astype(jnp.float32)
            for i in range(local):
                line = places[j, i : i + 1, :]
                onehot[lane, i * capacity : (i + 1) * capacity, :] = jnp.where(
                    line == ranks, 1.0, 0.0
                ).astype(jnp.bfloat16)

        half = slots // 2
        for h in range(2):
            picked = jnp.dot(
                onehot[lane, h * half : (h + 1) * half, :],
                blocks[j, c],
                preferred_element_type=jnp.float32,
            ).astype(jnp.bfloat16)
            dbuf[j, c, h * half : (h + 1) * half, :] = picked

        def give(d, carry):
            i = lax.rem(mine + d, local)
            sent(
                dbuf.at[j, c, pl.ds(i * capacity, capacity)],
                inc.at[j, c, g, pl.ds(y * capacity, capacity)],
                ps,
                pr.at[j, c],
                (z * SIDES + i // gates, lax.rem(i, gates)),
            ).start()
            return carry

        lax.fori_loop(1, local, give, 0)
        copied(
            dbuf.at[j, c, pl.ds(mine * capacity, capacity)],
            inc.at[j, c, g, pl.ds(y * capacity, capacity)],
            pr.at[j, c],
        ).start()

    def expert(t):
        p, c = item(t)
        j = block_at(p)
        lane = lax.rem(p, 2)
        copied(inc.at[j, c], inc.at[j, c], pr.at[j, c]).wait()
        share = width * chunks
        tile = 256
        for n in range(hidden.shape[2] // tile):
            cols = slice(n * tile, (n + 1) * tile)
            acc = jnp.zeros((SIDES * capacity, tile), jnp.float32)
            for k in range(gates):
                start = pl.multiple_of(k * share + c * width, width)
                acc += jnp.dot(
                    inc[j, c, k], upv[pl.ds(start, width), cols], preferred_element_type=jnp.float32
                )

            @pl.when(c == 0)
            def _():
                hidden[lane, :, cols] = acc

            @pl.when(c != 0)
            def _():
                hidden[lane, :, cols] += acc

        @pl.when(c == chunks - 1)
        def _():
            active = jnp.maximum(hidden[lane], 0.0).astype(jnp.bfloat16)
            out_width = downv.shape[1] // gates
            for k in range(gates):
                out = jnp.dot(
                    active,
                    downv[:, k * out_width : (k + 1) * out_width],
                    preferred_element_type=jnp.float32,
                ).astype(jnp.bfloat16)
                obuf[j, k] = out

            @pl.when(jnp.logical_not(held_back(j)))
            def _():
                give_back(j)

    def step(t, carry):
        @pl.when(t < items)
        def _():
            dispatch(t)

        @pl.when(t == 1)
        def _():
            for copy in gate_routes:
                copy.start()
            for copy in weights:
                copy.wait()

        @pl.when(t >= 1)
        def _():
            expert(t - 1)

        return carry

    lax.fori_loop(0, items + 1, step, 0)

    for c in range(chunks):

        @pl.when(up_ok)
        def _():
            shift(z, c, zs_up.at[c], 1).wait_send()

        @pl.when(down_ok)
        def _():
            shift(z, c, zs_down.at[c], -1).wait_send()

    def relayed(t, carry):
        j, c = t // chunks, lax.rem(t, chunks)

        @pl.when(relay_up(j) | relay_down(j))
        def _():
            copied(blocks.at[j, c], blocks.at[j, c], zs_relay.at[j, c]).wait()

        return carry

    lax.fori_loop(0, items, relayed, 0)

    @pl.when(up_ok & down_ok)
    def _():
        for j in (0, planes - 1):
            give_back(j)

    for copy in routes + gate_routes:
        copy.wait_send()
    for copy in gate_routes:
        copy.wait_recv()
    given = dbuf.at[:, :, pl.ds(0, slots - capacity)]
    copied(given, given, ps).wait()
    handed = ret.at[pl.ds(0, total - 1)]
    copied(handed, handed, rs).wait()

    def arrived(i, carry):
        copied(ret.at[i], ret.at[i], rr.at[i]).wait()
        return carry

    lax.fori_loop(0, total, arrived, 0)


def exchange(samples, place, gate_weight, up, down, planes, gates, capacity):
    rows, share = samples.shape
    local = SIDES * gates
    total = planes * local
    width = share // CHUNKS
    depth, inner = up.shape[1:]
    outer = down.shape[2]
    out_width = outer // gates
    bf16, f32 = jnp.bfloat16, jnp.float32
    dma = pltpu.SemaphoreType.DMA
    vmem = pl.BlockSpec(memory_space=pltpu.VMEM)
    hbm = pl.BlockSpec(memory_space=pl.ANY)
    return pl.pallas_call(
        functools.partial(exchange_kernel, planes, gates, capacity),
        out_shape=(
            jax.ShapeDtypeStruct((total, capacity, out_width), bf16),
            jax.ShapeDtypeStruct((gates, total, rows), f32),
        ),
        in_specs=[hbm, vmem, vmem, hbm, hbm],
        out_specs=(vmem, vmem),
        scratch_shapes=[
            pltpu.VMEM((planes, CHUNKS, rows, width), bf16),
            pltpu.VMEM((planes, local, rows), f32),
            pltpu.VMEM((2, local * capacity, rows), bf16),
            pltpu.VMEM((planes, CHUNKS, local * capacity, width), bf16),
            pltpu.VMEM((planes, CHUNKS, gates, SIDES * capacity, width), bf16),
            pltpu.VMEM((depth, inner), bf16),
            pltpu.VMEM((inner, outer), bf16),
            pltpu.VMEM((2, SIDES * capacity, inner), f32),
            pltpu.VMEM((planes, gates, SIDES * capacity, out_width), bf16),
            dma((CHUNKS,)),
            dma((2,)),
            dma((CHUNKS,)),
            dma((CHUNKS,)),
            dma((planes, CHUNKS)),
            dma((planes, CHUNKS)),
            dma,
            dma((planes, CHUNKS)),
            dma,
            dma((total,)),
            dma((planes,)),
            dma((planes,)),
            dma((gates,)),
            dma((gates,)),
            dma,
        ],
        compiler_params=pltpu.CompilerParams(
            collective_id=0, has_side_effects=True, vmem_limit_bytes=56 << 20
        ),
    )(samples, place, gate_weight, up, down)


def combine(returned, expert_ids, first, second, before, factor0, factor1, capacity):
    slots = jnp.arange(returned.shape[0], dtype=jnp.int32)[None, :]
    mixed = 0.0
    for k, (chosen, factor) in enumerate(((first, factor0), (second, factor1))):
        rank = jnp.sum(jnp.where(chosen, before, 0), axis=1, keepdims=True)
        position = expert_ids[:, k : k + 1] * capacity + rank
        pick = (position == slots).astype(jnp.bfloat16)
        mixed += factor * jnp.dot(pick, returned, preferred_element_type=jnp.float32)
    return mixed.astype(jnp.bfloat16)


def in_one_kernel(samples, gate_weight, expert_ids, pad_mask, up_weight, down_weight):
    group_count = lax.axis_size("expert")
    gate_count = lax.axis_size("gate")
    expert_count = group_count * gate_count
    capacity = 4 * samples.shape[0] // expert_count
    first, second, member, before = routing(expert_ids, expert_count)
    place = jnp.where(member, before, -1).T.astype(jnp.float32)
    returned, logits = exchange(
        samples,
        place,
        gate_weight.T,
        up_weight,
        down_weight,
        group_count // SIDES,
        gate_count,
        capacity,
    )
    returned = returned.reshape(expert_count * capacity, -1)
    logits = jnp.sum(logits, axis=0).T
    factor0, factor1 = factors(logits, first, second, pad_mask, expert_count)
    return combine(returned, expert_ids, first, second, before, factor0, factor1, capacity)


def fits(samples, up_weight, down_weight):
    group_count = lax.axis_size("expert")
    capacity = 4 * samples.shape[0] // (group_count * lax.axis_size("gate"))
    planes = group_count // SIDES
    held = 2 * (planes * samples.size * 3 + up_weight.size + down_weight.size)
    return group_count % SIDES == 0 and capacity % 16 == 0 and held < 40 << 20


def per_device(samples, gate_weight, expert_ids, pad_mask, up_weight, down_weight):
    if fits(samples, up_weight, down_weight):
        return in_one_kernel(
            samples, gate_weight, expert_ids, pad_mask, up_weight, down_weight
        )
    row_count, share = samples.shape
    group_count = lax.axis_size("expert")
    gate_count = lax.axis_size("gate")
    expert_count = group_count * gate_count
    capacity = 4 * row_count // expert_count
    partial = jnp.dot(samples, gate_weight, preferred_element_type=jnp.float32)
    logits = jnp.sum(lax.all_gather(partial, "gate"), axis=0)
    first, second, member, before = routing(expert_ids, expert_count)
    place = jnp.where(member, before, -1).T
    ranks = jnp.arange(capacity, dtype=jnp.int32)
    send = (place[:, None, :] == ranks[None, :, None]).astype(jnp.bfloat16)
    outgoing = jnp.dot(
        send.reshape(expert_count * capacity, row_count), samples, preferred_element_type=jnp.float32
    ).astype(jnp.bfloat16)
    incoming = lax.all_to_all(
        outgoing.reshape(expert_count, capacity, share),
        ("expert", "gate"),
        split_axis=0,
        concat_axis=0,
        tiled=True,
    ).reshape(group_count, gate_count, capacity, share)
    hidden = 0.0
    for g in range(gate_count):
        hidden += jnp.dot(
            incoming[:, g].reshape(group_count * capacity, share),
            up_weight[0, g * share : (g + 1) * share],
            preferred_element_type=jnp.float32,
        )
    active = jnp.maximum(hidden, 0.0).astype(jnp.bfloat16)
    expert_out = jnp.dot(active, down_weight[0], preferred_element_type=jnp.float32).astype(
        jnp.bfloat16
    )
    out_share = expert_out.shape[1] // gate_count
    outbound = expert_out.reshape(group_count, capacity, gate_count, out_share)
    outbound = outbound.transpose(0, 2, 1, 3).reshape(expert_count, capacity, out_share)
    returned = lax.all_to_all(
        outbound, ("expert", "gate"), split_axis=0, concat_axis=0, tiled=True
    ).reshape(expert_count * capacity, out_share)
    factor0, factor1 = factors(logits, first, second, pad_mask, expert_count)
    slots = jnp.arange(expert_count * capacity, dtype=jnp.int32)[None, :]
    mixed = 0.0
    for k, (chosen, factor) in enumerate(((first, factor0), (second, factor1))):
        rank = jnp.sum(jnp.where(chosen, before, 0), axis=1, keepdims=True)
        position = expert_ids[:, k : k + 1] * capacity + rank
        pick = (position == slots).astype(jnp.bfloat16)
        mixed += factor * jnp.dot(pick, returned, preferred_element_type=jnp.float32)
    return mixed.astype(jnp.bfloat16)


def solution(mesh):
    placed = (
        P("expert", "gate"),
        P("gate", None),
        P("expert", None),
        P("expert"),
        P(("expert", "gate"), None, None),
        P(("expert", "gate"), None, None),
    )
    return jax.shard_map(
        per_device, mesh=mesh, in_specs=placed, out_specs=P("expert", "gate"), check_vma=False
    )
```

```python
import functools

import jax
import jax.numpy as jnp
from jax import lax
from jax.experimental import pallas as pl
from jax.experimental.pallas import tpu as pltpu
from jax.sharding import PartitionSpec as P


MESH = pl.DeviceIdType.MESH
CHUNKS = 4
SIDES = 2


def routing(expert_ids, expert_count):
    row_count = expert_ids.shape[0]
    lanes = jnp.arange(expert_count, dtype=jnp.int32)[None, :]
    first = expert_ids[:, 0:1] == lanes
    second = expert_ids[:, 1:2] == lanes
    member = first | second
    rows = jnp.arange(row_count, dtype=jnp.int32)
    lower = (rows[:, None] > rows[None, :]).astype(jnp.bfloat16)
    before = jnp.dot(lower, member.astype(jnp.bfloat16), preferred_element_type=jnp.float32)
    before = before.astype(jnp.int32)
    return first, second, member, before


def factors(logits, first, second, pad_mask, expert_count):
    top = jnp.max(logits, axis=1, keepdims=True)
    terms = jnp.exp(logits - top)
    scale = pad_mask.astype(jnp.float32)[:, None] / jnp.sum(terms, axis=1, keepdims=True)
    factor0 = expert_count * jnp.sum(jnp.where(first, terms, 0.0), axis=1, keepdims=True) * scale
    factor1 = expert_count * jnp.sum(jnp.where(second, terms, 0.0), axis=1, keepdims=True) * scale
    return factor0, factor1


def copied(source, target, sem):
    return pltpu.make_async_copy(source, target, sem)


def sent(source, target, send_sem, recv_sem, device):
    return pltpu.make_async_remote_copy(
        src_ref=source,
        dst_ref=target,
        send_sem=send_sem,
        recv_sem=recv_sem,
        device_id=device,
        device_id_type=MESH,
    )


def table(values, index):
    out = values[0]
    for k in range(1, len(values)):
        out = jnp.where(index == k, values[k], out)
    return out


def exchange_kernel(
    planes,
    gates,
    capacity,
    samples,
    ids,
    mask,
    gate_weight,
    up,
    down,
    mixed,
    ret,
    logits,
    place,
    factor,
    blocks,
    places,
    onehot,
    dbuf,
    inc,
    upv,
    downv,
    hidden,
    obuf,
    own_sem,
    w_sem,
    zs_up,
    zs_down,
    zs_relay,
    zr,
    ps,
    pr,
    rs,
    rr,
    ms,
    mr,
    gs,
    gr,
    l_sem,
):
    chunks = CHUNKS
    local = SIDES * gates
    e = lax.axis_index("expert")
    g = lax.axis_index("gate")
    z = e // SIDES
    y = lax.rem(e, SIDES)
    mine = y * gates + g
    me = e * gates + g
    total = planes * local
    rows = blocks.shape[2]
    width = blocks.shape[3]
    slots = local * capacity

    own = [
        copied(samples.at[:, pl.ds(c * width, width)], blocks.at[z, c], own_sem.at[c])
        for c in range(chunks)
    ]
    for copy in own:
        copy.start()
    weights = (copied(up.at[0], upv, w_sem.at[0]), copied(down.at[0], downv, w_sem.at[1]))

    barrier = pltpu.get_barrier_semaphore()

    def greet(d, carry):
        t = lax.rem(me + d, total)
        pl.semaphore_signal(
            barrier, inc=1, device_id=(t // gates, lax.rem(t, gates)), device_id_type=MESH
        )
        return carry

    lax.fori_loop(1, total, greet, 0)
    pl.semaphore_wait(barrier, total - 1)

    up_ok = z + 1 < planes
    down_ok = z >= 1

    def shift(j, c, sem, step):
        return sent(
            blocks.at[j, c], blocks.at[j, c], sem, zr.at[j, c], ((z + step) * SIDES + y, g)
        )

    for c in range(chunks):
        own[c].wait()

        @pl.when(up_ok)
        def _():
            shift(z, c, zs_up.at[c], 1).start()

        @pl.when(down_ok)
        def _():
            shift(z, c, zs_down.at[c], -1).start()

    lanes = lax.broadcasted_iota(jnp.int32, (total, rows), 0)
    member = (ids[0:1, :] == lanes) | (ids[1:2, :] == lanes)
    earlier = lax.broadcasted_iota(jnp.int32, (rows, rows), 0) < lax.broadcasted_iota(
        jnp.int32, (rows, rows), 1
    )
    before = jnp.dot(
        jnp.where(member, 1.0, 0.0).astype(jnp.bfloat16),
        jnp.where(earlier, 1.0, 0.0).astype(jnp.bfloat16),
        preferred_element_type=jnp.float32,
    )
    place[...] = jnp.where(member, before, -1.0)
    for copy in weights:
        copy.start()
    partial = 0.0
    for c in range(chunks):
        partial += lax.dot_general(
            gate_weight[:, c * width : (c + 1) * width],
            blocks[z, c],
            (((1,), (1,)), ((), ())),
            preferred_element_type=jnp.float32,
        )
    logits[g] = partial
    routes = []
    for d in range(1, planes):
        j = lax.rem(z + d, planes)
        routes.append(
            sent(
                place.at[pl.ds(j * local, local)],
                places.at[z],
                ms.at[d - 1],
                mr.at[z],
                (j * SIDES + y, g),
            )
        )
        routes[-1].start()
    kept = copied(place.at[pl.ds(z * local, local)], places.at[z], l_sem)
    kept.start()
    kept.wait()
    gate_routes = []
    for d in range(1, gates):
        t = lax.rem(g + d, gates)
        gate_routes.append(sent(logits.at[g], logits.at[g], gs.at[d - 1], gr.at[d - 1], (e, t)))

    orders = [sorted(range(planes), key=lambda j: (abs(j - k), j)) for k in range(planes)]

    def block_at(p):
        return table([table(order, p) for order in orders], z)

    def relay_up(j):
        return (j < z) & up_ok

    def relay_down(j):
        return (j > z) & down_ok

    items = planes * chunks

    def held_back(j):
        return up_ok & down_ok & ((j == 0) | (j == planes - 1))

    def give_back(j):
        def hand(i, carry):
            side, k = i // gates, lax.rem(i, gates)
            block = obuf.at[j, k, pl.ds(side * capacity, capacity)]
            away = (j != z) | (i != mine)

            @pl.when(away)
            def _():
                sent(block, ret.at[me], rs, rr.at[me], (j * SIDES + side, k)).start()

            @pl.when(jnp.logical_not(away))
            def _():
                copied(block, ret.at[me], rr.at[me]).start()

            return carry

        lax.fori_loop(0, local, hand, 0)

    def item(t):
        u = t - chunks
        in_turn = up_ok & down_ok & (u >= 0) & (u < 2 * chunks)
        p = jnp.where(in_turn, 1 + lax.rem(u + 2 * chunks, 2), t // chunks)
        return p, jnp.where(in_turn, u // 2, lax.rem(t, chunks))

    def dispatch(t):
        p, c = item(t)
        j = block_at(p)
        lane = lax.rem(p, 2)

        @pl.when(j != z)
        def _():
            copied(blocks.at[j, c], blocks.at[j, c], zr.at[j, c]).wait()

            @pl.when(relay_up(j))
            def _():
                shift(j, c, zs_relay.at[j, c], 1).start()

            @pl.when(relay_down(j))
            def _():
                shift(j, c, zs_relay.at[j, c], -1).start()

        @pl.when(c == 0)
        def _():
            @pl.when(j != z)
            def _():
                copied(places.at[j], places.at[j], mr.at[j]).wait()

            ranks = lax.broadcasted_iota(jnp.int32, (capacity, rows), 0).astype(jnp.float32)
            for i in range(local):
                line = places[j, i : i + 1, :]
                onehot[lane, i * capacity : (i + 1) * capacity, :] = jnp.where(
                    line == ranks, 1.0, 0.0
                ).astype(jnp.bfloat16)

        half = slots // 2
        for h in range(2):
            picked = jnp.dot(
                onehot[lane, h * half : (h + 1) * half, :],
                blocks[j, c],
                preferred_element_type=jnp.float32,
            ).astype(jnp.bfloat16)
            dbuf[j, c, h * half : (h + 1) * half, :] = picked

        def give(d, carry):
            i = lax.rem(mine + d, local)
            sent(
                dbuf.at[j, c, pl.ds(i * capacity, capacity)],
                inc.at[j, c, g, pl.ds(y * capacity, capacity)],
                ps,
                pr.at[j, c],
                (z * SIDES + i // gates, lax.rem(i, gates)),
            ).start()
            return carry

        lax.fori_loop(1, local, give, 0)
        copied(
            dbuf.at[j, c, pl.ds(mine * capacity, capacity)],
            inc.at[j, c, g, pl.ds(y * capacity, capacity)],
            pr.at[j, c],
        ).start()

    def expert(t):
        p, c = item(t)
        j = block_at(p)
        lane = lax.rem(p, 2)
        copied(inc.at[j, c], inc.at[j, c], pr.at[j, c]).wait()
        share = width * chunks
        tile = 256
        for n in range(hidden.shape[2] // tile):
            cols = slice(n * tile, (n + 1) * tile)
            acc = jnp.zeros((SIDES * capacity, tile), jnp.float32)
            for k in range(gates):
                start = pl.multiple_of(k * share + c * width, width)
                acc += jnp.dot(
                    inc[j, c, k], upv[pl.ds(start, width), cols], preferred_element_type=jnp.float32
                )

            @pl.when(c == 0)
            def _():
                hidden[lane, :, cols] = acc

            @pl.when(c != 0)
            def _():
                hidden[lane, :, cols] += acc

        @pl.when(c == chunks - 1)
        def _():
            active = jnp.maximum(hidden[lane], 0.0).astype(jnp.bfloat16)
            out_width = downv.shape[1] // gates
            for k in range(gates):
                out = jnp.dot(
                    active,
                    downv[:, k * out_width : (k + 1) * out_width],
                    preferred_element_type=jnp.float32,
                ).astype(jnp.bfloat16)
                obuf[j, k] = out

            @pl.when(jnp.logical_not(held_back(j)))
            def _():
                give_back(j)

    def step(t, carry):
        @pl.when(t < items)
        def _():
            dispatch(t)

        @pl.when(t == 1)
        def _():
            for copy in gate_routes:
                copy.start()
            for copy in weights:
                copy.wait()

        @pl.when(t >= 1)
        def _():
            expert(t - 1)

        return carry

    lax.fori_loop(0, items + 1, step, 0)

    for c in range(chunks):

        @pl.when(up_ok)
        def _():
            shift(z, c, zs_up.at[c], 1).wait_send()

        @pl.when(down_ok)
        def _():
            shift(z, c, zs_down.at[c], -1).wait_send()

    def relayed(t, carry):
        j, c = t // chunks, lax.rem(t, chunks)

        @pl.when(relay_up(j) | relay_down(j))
        def _():
            copied(blocks.at[j, c], blocks.at[j, c], zs_relay.at[j, c]).wait()

        return carry

    lax.fori_loop(0, items, relayed, 0)

    @pl.when(up_ok & down_ok)
    def _():
        for j in (0, planes - 1):
            give_back(j)

    for copy in routes + gate_routes:
        copy.wait_send()
    for copy in gate_routes:
        copy.wait_recv()
    logit = logits[0]
    for k in range(1, gates):
        logit += logits[k]
    terms = jnp.exp(logit - jnp.max(logit, axis=0, keepdims=True))
    scale = total * mask[...].astype(jnp.float32) / jnp.sum(terms, axis=0, keepdims=True)
    factor[...] = jnp.where(place[...] >= 0.0, terms * scale, 0.0)

    def collect(p, carry):
        j = block_at(p)
        start = pl.multiple_of(j * local, local)
        places[j] = place[pl.ds(start, local), :]
        weight = factor[pl.ds(start, local), :]
        ranks = lax.broadcasted_iota(jnp.int32, (capacity, rows), 0).astype(jnp.float32)
        for i in range(local):
            chosen = places[j, i : i + 1, :] == ranks
            exact = weight[i : i + 1, :]
            high = exact.astype(jnp.bfloat16).astype(jnp.float32)
            span = slice(i * capacity, (i + 1) * capacity)
            onehot[0, span, :] = jnp.where(chosen, high, 0.0).astype(jnp.bfloat16)
            onehot[1, span, :] = jnp.where(chosen, exact - high, 0.0).astype(jnp.bfloat16)

        def arrived(i, inner):
            copied(ret.at[start + i], ret.at[start + i], rr.at[start + i]).wait()
            return inner

        lax.fori_loop(0, local, arrived, 0)
        back = ret[pl.ds(start, local)].reshape(slots, ret.shape[2])
        part = 0.0
        for k in range(2):
            part += lax.dot_general(
                onehot[k], back, (((0,), (0,)), ((), ())), preferred_element_type=jnp.float32
            )

        @pl.when(p == 0)
        def _():
            mixed[...] = part

        @pl.when(p != 0)
        def _():
            mixed[...] += part

        return carry

    lax.fori_loop(0, planes, collect, 0)
    given = dbuf.at[:, :, pl.ds(0, slots - capacity)]
    copied(given, given, ps).wait()
    handed = ret.at[pl.ds(0, total - 1)]
    copied(handed, handed, rs).wait()


def exchange(samples, ids, mask, gate_weight, up, down, planes, gates, capacity):
    rows, share = samples.shape
    local = SIDES * gates
    total = planes * local
    width = share // CHUNKS
    depth, inner = up.shape[1:]
    outer = down.shape[2]
    out_width = outer // gates
    bf16, f32 = jnp.bfloat16, jnp.float32
    dma = pltpu.SemaphoreType.DMA
    vmem = pl.BlockSpec(memory_space=pltpu.VMEM)
    hbm = pl.BlockSpec(memory_space=pl.ANY)
    return pl.pallas_call(
        functools.partial(exchange_kernel, planes, gates, capacity),
        out_shape=jax.ShapeDtypeStruct((rows, out_width), f32),
        in_specs=[hbm, vmem, vmem, vmem, hbm, hbm],
        out_specs=vmem,
        scratch_shapes=[
            pltpu.VMEM((total, capacity, out_width), bf16),
            pltpu.VMEM((gates, total, rows), f32),
            pltpu.VMEM((total, rows), f32),
            pltpu.VMEM((total, rows), f32),
            pltpu.VMEM((planes, CHUNKS, rows, width), bf16),
            pltpu.VMEM((planes, local, rows), f32),
            pltpu.VMEM((2, local * capacity, rows), bf16),
            pltpu.VMEM((planes, CHUNKS, local * capacity, width), bf16),
            pltpu.VMEM((planes, CHUNKS, gates, SIDES * capacity, width), bf16),
            pltpu.VMEM((depth, inner), bf16),
            pltpu.VMEM((inner, outer), bf16),
            pltpu.VMEM((2, SIDES * capacity, inner), f32),
            pltpu.VMEM((planes, gates, SIDES * capacity, out_width), bf16),
            dma((CHUNKS,)),
            dma((2,)),
            dma((CHUNKS,)),
            dma((CHUNKS,)),
            dma((planes, CHUNKS)),
            dma((planes, CHUNKS)),
            dma,
            dma((planes, CHUNKS)),
            dma,
            dma((total,)),
            dma((planes,)),
            dma((planes,)),
            dma((gates,)),
            dma((gates,)),
            dma,
        ],
        compiler_params=pltpu.CompilerParams(
            collective_id=0, has_side_effects=True, vmem_limit_bytes=56 << 20
        ),
    )(samples, ids, mask, gate_weight, up, down)


def in_one_kernel(samples, gate_weight, expert_ids, pad_mask, up_weight, down_weight):
    group_count = lax.axis_size("expert")
    gate_count = lax.axis_size("gate")
    capacity = 4 * samples.shape[0] // (group_count * gate_count)
    mixed = exchange(
        samples,
        expert_ids.T,
        pad_mask[None, :],
        gate_weight.T,
        up_weight,
        down_weight,
        group_count // SIDES,
        gate_count,
        capacity,
    )
    return mixed.astype(jnp.bfloat16)


def fits(samples, up_weight, down_weight):
    group_count = lax.axis_size("expert")
    capacity = 4 * samples.shape[0] // (group_count * lax.axis_size("gate"))
    planes = group_count // SIDES
    held = 2 * (planes * samples.size * 3 + up_weight.size + down_weight.size)
    return group_count % SIDES == 0 and capacity % 16 == 0 and held < 40 << 20


def per_device(samples, gate_weight, expert_ids, pad_mask, up_weight, down_weight):
    if fits(samples, up_weight, down_weight):
        return in_one_kernel(
            samples, gate_weight, expert_ids, pad_mask, up_weight, down_weight
        )
    row_count, share = samples.shape
    group_count = lax.axis_size("expert")
    gate_count = lax.axis_size("gate")
    expert_count = group_count * gate_count
    capacity = 4 * row_count // expert_count
    partial = jnp.dot(samples, gate_weight, preferred_element_type=jnp.float32)
    logits = jnp.sum(lax.all_gather(partial, "gate"), axis=0)
    first, second, member, before = routing(expert_ids, expert_count)
    place = jnp.where(member, before, -1).T
    ranks = jnp.arange(capacity, dtype=jnp.int32)
    send = (place[:, None, :] == ranks[None, :, None]).astype(jnp.bfloat16)
    outgoing = jnp.dot(
        send.reshape(expert_count * capacity, row_count), samples, preferred_element_type=jnp.float32
    ).astype(jnp.bfloat16)
    incoming = lax.all_to_all(
        outgoing.reshape(expert_count, capacity, share),
        ("expert", "gate"),
        split_axis=0,
        concat_axis=0,
        tiled=True,
    ).reshape(group_count, gate_count, capacity, share)
    hidden = 0.0
    for g in range(gate_count):
        hidden += jnp.dot(
            incoming[:, g].reshape(group_count * capacity, share),
            up_weight[0, g * share : (g + 1) * share],
            preferred_element_type=jnp.float32,
        )
    active = jnp.maximum(hidden, 0.0).astype(jnp.bfloat16)
    expert_out = jnp.dot(active, down_weight[0], preferred_element_type=jnp.float32).astype(
        jnp.bfloat16
    )
    out_share = expert_out.shape[1] // gate_count
    outbound = expert_out.reshape(group_count, capacity, gate_count, out_share)
    outbound = outbound.transpose(0, 2, 1, 3).reshape(expert_count, capacity, out_share)
    returned = lax.all_to_all(
        outbound, ("expert", "gate"), split_axis=0, concat_axis=0, tiled=True
    ).reshape(expert_count * capacity, out_share)
    factor0, factor1 = factors(logits, first, second, pad_mask, expert_count)
    slots = jnp.arange(expert_count * capacity, dtype=jnp.int32)[None, :]
    mixed = 0.0
    for k, (chosen, factor) in enumerate(((first, factor0), (second, factor1))):
        rank = jnp.sum(jnp.where(chosen, before, 0), axis=1, keepdims=True)
        position = expert_ids[:, k : k + 1] * capacity + rank
        pick = (position == slots).astype(jnp.bfloat16)
        mixed += factor * jnp.dot(pick, returned, preferred_element_type=jnp.float32)
    return mixed.astype(jnp.bfloat16)


def solution(mesh):
    placed = (
        P("expert", "gate"),
        P("gate", None),
        P("expert", None),
        P("expert"),
        P(("expert", "gate"), None, None),
        P(("expert", "gate"), None, None),
    )
    return jax.shard_map(
        per_device, mesh=mesh, in_specs=placed, out_specs=P("expert", "gate"), check_vma=False
    )
```

```python
import functools

import jax
import jax.numpy as jnp
from jax import lax
from jax.experimental import pallas as pl
from jax.experimental.pallas import tpu as pltpu
from jax.sharding import PartitionSpec as P


MESH = pl.DeviceIdType.MESH
CHUNKS = 4
SIDES = 2


def routing(expert_ids, expert_count):
    row_count = expert_ids.shape[0]
    lanes = jnp.arange(expert_count, dtype=jnp.int32)[None, :]
    first = expert_ids[:, 0:1] == lanes
    second = expert_ids[:, 1:2] == lanes
    member = first | second
    rows = jnp.arange(row_count, dtype=jnp.int32)
    lower = (rows[:, None] > rows[None, :]).astype(jnp.bfloat16)
    before = jnp.dot(lower, member.astype(jnp.bfloat16), preferred_element_type=jnp.float32)
    before = before.astype(jnp.int32)
    return first, second, member, before


def factors(logits, first, second, pad_mask, expert_count):
    top = jnp.max(logits, axis=1, keepdims=True)
    terms = jnp.exp(logits - top)
    scale = pad_mask.astype(jnp.float32)[:, None] / jnp.sum(terms, axis=1, keepdims=True)
    factor0 = expert_count * jnp.sum(jnp.where(first, terms, 0.0), axis=1, keepdims=True) * scale
    factor1 = expert_count * jnp.sum(jnp.where(second, terms, 0.0), axis=1, keepdims=True) * scale
    return factor0, factor1


def copied(source, target, sem):
    return pltpu.make_async_copy(source, target, sem)


def sent(source, target, send_sem, recv_sem, device):
    return pltpu.make_async_remote_copy(
        src_ref=source,
        dst_ref=target,
        send_sem=send_sem,
        recv_sem=recv_sem,
        device_id=device,
        device_id_type=MESH,
    )


def table(values, index):
    out = values[0]
    for k in range(1, len(values)):
        out = jnp.where(index == k, values[k], out)
    return out


def exchange_kernel(
    planes,
    gates,
    capacity,
    samples,
    ids,
    mask,
    gate_weight,
    up,
    down,
    mixed,
    ret,
    logits,
    place,
    factor,
    blocks,
    places,
    onehot,
    dbuf,
    inc,
    upv,
    downv,
    hidden,
    obuf,
    own_sem,
    w_sem,
    zs_up,
    zs_down,
    zs_relay,
    zr,
    ps,
    pr,
    rs,
    rr,
    ms,
    mr,
    gs,
    gr,
    l_sem,
):
    chunks = CHUNKS
    local = SIDES * gates
    e = lax.axis_index("expert")
    g = lax.axis_index("gate")
    z = e // SIDES
    y = lax.rem(e, SIDES)
    mine = y * gates + g
    me = e * gates + g
    total = planes * local
    rows = blocks.shape[2]
    width = blocks.shape[3]
    slots = local * capacity

    own = [
        copied(samples.at[:, pl.ds(c * width, width)], blocks.at[z, c], own_sem.at[c])
        for c in range(chunks)
    ]
    for copy in own:
        copy.start()
    weights = (copied(up.at[0], upv, w_sem.at[0]), copied(down.at[0], downv, w_sem.at[1]))

    barrier = pltpu.get_barrier_semaphore()

    def greet(d, carry):
        t = lax.rem(me + d, total)
        pl.semaphore_signal(
            barrier, inc=1, device_id=(t // gates, lax.rem(t, gates)), device_id_type=MESH
        )
        return carry

    lax.fori_loop(1, total, greet, 0)
    pl.semaphore_wait(barrier, total - 1)

    up_ok = z + 1 < planes
    down_ok = z >= 1

    def shift(j, c, sem, step):
        return sent(
            blocks.at[j, c], blocks.at[j, c], sem, zr.at[j, c], ((z + step) * SIDES + y, g)
        )

    for c in range(chunks):
        own[c].wait()

        @pl.when(up_ok)
        def _():
            shift(z, c, zs_up.at[c], 1).start()

        @pl.when(down_ok)
        def _():
            shift(z, c, zs_down.at[c], -1).start()

    lanes = lax.broadcasted_iota(jnp.int32, (total, rows), 0)
    member = (ids[0:1, :] == lanes) | (ids[1:2, :] == lanes)
    earlier = lax.broadcasted_iota(jnp.int32, (rows, rows), 0) < lax.broadcasted_iota(
        jnp.int32, (rows, rows), 1
    )
    before = jnp.dot(
        jnp.where(member, 1.0, 0.0).astype(jnp.bfloat16),
        jnp.where(earlier, 1.0, 0.0).astype(jnp.bfloat16),
        preferred_element_type=jnp.float32,
    )
    place[...] = jnp.where(member, before, -1.0)
    for copy in weights:
        copy.start()
    partial = 0.0
    for c in range(chunks):
        partial += lax.dot_general(
            gate_weight[:, c * width : (c + 1) * width],
            blocks[z, c],
            (((1,), (1,)), ((), ())),
            preferred_element_type=jnp.float32,
        )
    logits[g] = partial
    routes = []
    for d in range(1, planes):
        j = lax.rem(z + d, planes)
        routes.append(
            sent(
                place.at[pl.ds(j * local, local)],
                places.at[z],
                ms.at[d - 1],
                mr.at[z],
                (j * SIDES + y, g),
            )
        )
        routes[-1].start()
    kept = copied(place.at[pl.ds(z * local, local)], places.at[z], l_sem)
    kept.start()
    kept.wait()
    gate_routes = []
    for d in range(1, gates):
        t = lax.rem(g + d, gates)
        gate_routes.append(sent(logits.at[g], logits.at[g], gs.at[d - 1], gr.at[d - 1], (e, t)))

    orders = [sorted(range(planes), key=lambda j: (abs(j - k), j)) for k in range(planes)]

    def block_at(p):
        return table([table(order, p) for order in orders], z)

    def relay_up(j):
        return (j < z) & up_ok

    def relay_down(j):
        return (j > z) & down_ok

    items = planes * chunks

    def held_back(j):
        return up_ok & down_ok & ((j == 0) | (j == planes - 1))

    def give_back(j):
        def hand(i, carry):
            side, k = i // gates, lax.rem(i, gates)
            block = obuf.at[j, k, pl.ds(side * capacity, capacity)]
            away = (j != z) | (i != mine)

            @pl.when(away)
            def _():
                sent(block, ret.at[me], rs, rr.at[me], (j * SIDES + side, k)).start()

            @pl.when(jnp.logical_not(away))
            def _():
                copied(block, ret.at[me], rr.at[me]).start()

            return carry

        lax.fori_loop(0, local, hand, 0)

    def item(t):
        u = t - chunks
        in_turn = up_ok & down_ok & (u >= 0) & (u < 2 * chunks)
        p = jnp.where(in_turn, 1 + lax.rem(u + 2 * chunks, 2), t // chunks)
        return p, jnp.where(in_turn, u // 2, lax.rem(t, chunks))

    def dispatch(t):
        p, c = item(t)
        j = block_at(p)
        lane = lax.rem(p, 2)

        @pl.when(j != z)
        def _():
            copied(blocks.at[j, c], blocks.at[j, c], zr.at[j, c]).wait()

            @pl.when(relay_up(j))
            def _():
                shift(j, c, zs_relay.at[j, c], 1).start()

            @pl.when(relay_down(j))
            def _():
                shift(j, c, zs_relay.at[j, c], -1).start()

        @pl.when(c == 0)
        def _():
            @pl.when(j != z)
            def _():
                copied(places.at[j], places.at[j], mr.at[j]).wait()

            ranks = lax.broadcasted_iota(jnp.int32, (capacity, rows), 0).astype(jnp.float32)
            for i in range(local):
                line = places[j, i : i + 1, :]
                onehot[lane, i * capacity : (i + 1) * capacity, :] = jnp.where(
                    line == ranks, 1.0, 0.0
                ).astype(jnp.bfloat16)

        half = slots // 2
        for h in range(2):
            picked = jnp.dot(
                onehot[lane, h * half : (h + 1) * half, :],
                blocks[j, c],
                preferred_element_type=jnp.float32,
            ).astype(jnp.bfloat16)
            dbuf[j, c, h * half : (h + 1) * half, :] = picked

        def give(d, carry):
            i = lax.rem(mine + d, local)
            sent(
                dbuf.at[j, c, pl.ds(i * capacity, capacity)],
                inc.at[j, c, g, pl.ds(y * capacity, capacity)],
                ps,
                pr.at[j, c],
                (z * SIDES + i // gates, lax.rem(i, gates)),
            ).start()
            return carry

        lax.fori_loop(1, local, give, 0)
        copied(
            dbuf.at[j, c, pl.ds(mine * capacity, capacity)],
            inc.at[j, c, g, pl.ds(y * capacity, capacity)],
            pr.at[j, c],
        ).start()

    def expert(t):
        p, c = item(t)
        j = block_at(p)
        lane = lax.rem(p, 2)
        copied(inc.at[j, c], inc.at[j, c], pr.at[j, c]).wait()
        share = width * chunks
        tile = 256
        for n in range(hidden.shape[2] // tile):
            cols = slice(n * tile, (n + 1) * tile)
            acc = jnp.zeros((SIDES * capacity, tile), jnp.float32)
            for k in range(gates):
                start = pl.multiple_of(k * share + c * width, width)
                acc += jnp.dot(
                    inc[j, c, k], upv[pl.ds(start, width), cols], preferred_element_type=jnp.float32
                )

            @pl.when(c == 0)
            def _():
                hidden[lane, :, cols] = acc

            @pl.when(c != 0)
            def _():
                hidden[lane, :, cols] += acc

        @pl.when(c == chunks - 1)
        def _():
            active = jnp.maximum(hidden[lane], 0.0).astype(jnp.bfloat16)
            out_width = downv.shape[1] // gates
            for k in range(gates):
                out = jnp.dot(
                    active,
                    downv[:, k * out_width : (k + 1) * out_width],
                    preferred_element_type=jnp.float32,
                ).astype(jnp.bfloat16)
                obuf[j, k] = out

            @pl.when(jnp.logical_not(held_back(j)))
            def _():
                give_back(j)

    def step(t, carry):
        @pl.when(t < items)
        def _():
            dispatch(t)

        @pl.when(t == 1)
        def _():
            for copy in gate_routes:
                copy.start()
            for copy in weights:
                copy.wait()

        @pl.when(t >= 1)
        def _():
            expert(t - 1)

        return carry

    lax.fori_loop(0, items + 1, step, 0)

    for c in range(chunks):

        @pl.when(up_ok)
        def _():
            shift(z, c, zs_up.at[c], 1).wait_send()

        @pl.when(down_ok)
        def _():
            shift(z, c, zs_down.at[c], -1).wait_send()

    def relayed(t, carry):
        j, c = t // chunks, lax.rem(t, chunks)

        @pl.when(relay_up(j) | relay_down(j))
        def _():
            copied(blocks.at[j, c], blocks.at[j, c], zs_relay.at[j, c]).wait()

        return carry

    lax.fori_loop(0, items, relayed, 0)

    @pl.when(up_ok & down_ok)
    def _():
        for j in (0, planes - 1):
            give_back(j)

    for copy in routes + gate_routes:
        copy.wait_send()
    for copy in gate_routes:
        copy.wait_recv()
    logit = logits[0]
    for k in range(1, gates):
        logit += logits[k]
    terms = jnp.exp(logit - jnp.max(logit, axis=0, keepdims=True))
    scale = total * mask[...].astype(jnp.float32) / jnp.sum(terms, axis=0, keepdims=True)
    factor[...] = jnp.where(place[...] >= 0.0, terms * scale, 0.0)

    def collect(p, carry):
        j = block_at(p)
        start = pl.multiple_of(j * local, local)
        places[j] = place[pl.ds(start, local), :]
        weight = factor[pl.ds(start, local), :]
        ranks = lax.broadcasted_iota(jnp.int32, (capacity, rows), 0).astype(jnp.float32)
        for i in range(local):
            chosen = places[j, i : i + 1, :] == ranks
            exact = weight[i : i + 1, :]
            high = exact.astype(jnp.bfloat16).astype(jnp.float32)
            span = slice(i * capacity, (i + 1) * capacity)
            onehot[0, span, :] = jnp.where(chosen, high, 0.0).astype(jnp.bfloat16)
            onehot[1, span, :] = jnp.where(chosen, exact - high, 0.0).astype(jnp.bfloat16)

        def arrived(i, inner):
            copied(ret.at[start + i], ret.at[start + i], rr.at[start + i]).wait()
            return inner

        lax.fori_loop(0, local, arrived, 0)
        back = ret[pl.ds(start, local)].reshape(slots, ret.shape[2]).T
        part = 0.0
        for k in range(2):
            part += jnp.dot(back, onehot[k], preferred_element_type=jnp.float32)

        @pl.when(p == 0)
        def _():
            mixed[...] = part

        @pl.when(p != 0)
        def _():
            mixed[...] += part

        return carry

    lax.fori_loop(0, planes, collect, 0)
    given = dbuf.at[:, :, pl.ds(0, slots - capacity)]
    copied(given, given, ps).wait()
    handed = ret.at[pl.ds(0, total - 1)]
    copied(handed, handed, rs).wait()


def exchange(samples, ids, mask, gate_weight, up, down, planes, gates, capacity):
    rows, share = samples.shape
    local = SIDES * gates
    total = planes * local
    width = share // CHUNKS
    depth, inner = up.shape[1:]
    outer = down.shape[2]
    out_width = outer // gates
    bf16, f32 = jnp.bfloat16, jnp.float32
    dma = pltpu.SemaphoreType.DMA
    vmem = pl.BlockSpec(memory_space=pltpu.VMEM)
    hbm = pl.BlockSpec(memory_space=pl.ANY)
    return pl.pallas_call(
        functools.partial(exchange_kernel, planes, gates, capacity),
        out_shape=jax.ShapeDtypeStruct((out_width, rows), f32),
        in_specs=[hbm, vmem, vmem, vmem, hbm, hbm],
        out_specs=vmem,
        scratch_shapes=[
            pltpu.VMEM((total, capacity, out_width), bf16),
            pltpu.VMEM((gates, total, rows), f32),
            pltpu.VMEM((total, rows), f32),
            pltpu.VMEM((total, rows), f32),
            pltpu.VMEM((planes, CHUNKS, rows, width), bf16),
            pltpu.VMEM((planes, local, rows), f32),
            pltpu.VMEM((2, local * capacity, rows), bf16),
            pltpu.VMEM((planes, CHUNKS, local * capacity, width), bf16),
            pltpu.VMEM((planes, CHUNKS, gates, SIDES * capacity, width), bf16),
            pltpu.VMEM((depth, inner), bf16),
            pltpu.VMEM((inner, outer), bf16),
            pltpu.VMEM((2, SIDES * capacity, inner), f32),
            pltpu.VMEM((planes, gates, SIDES * capacity, out_width), bf16),
            dma((CHUNKS,)),
            dma((2,)),
            dma((CHUNKS,)),
            dma((CHUNKS,)),
            dma((planes, CHUNKS)),
            dma((planes, CHUNKS)),
            dma,
            dma((planes, CHUNKS)),
            dma,
            dma((total,)),
            dma((planes,)),
            dma((planes,)),
            dma((gates,)),
            dma((gates,)),
            dma,
        ],
        compiler_params=pltpu.CompilerParams(
            collective_id=0, has_side_effects=True, vmem_limit_bytes=56 << 20
        ),
    )(samples, ids, mask, gate_weight, up, down)


def in_one_kernel(samples, gate_weight, expert_ids, pad_mask, up_weight, down_weight):
    group_count = lax.axis_size("expert")
    gate_count = lax.axis_size("gate")
    capacity = 4 * samples.shape[0] // (group_count * gate_count)
    mixed = exchange(
        samples,
        expert_ids.T,
        pad_mask[None, :],
        gate_weight.T,
        up_weight,
        down_weight,
        group_count // SIDES,
        gate_count,
        capacity,
    )
    return mixed.T.astype(jnp.bfloat16)


def fits(samples, up_weight, down_weight):
    group_count = lax.axis_size("expert")
    capacity = 4 * samples.shape[0] // (group_count * lax.axis_size("gate"))
    planes = group_count // SIDES
    held = 2 * (planes * samples.size * 3 + up_weight.size + down_weight.size)
    return group_count % SIDES == 0 and capacity % 16 == 0 and held < 40 << 20


def per_device(samples, gate_weight, expert_ids, pad_mask, up_weight, down_weight):
    if fits(samples, up_weight, down_weight):
        return in_one_kernel(
            samples, gate_weight, expert_ids, pad_mask, up_weight, down_weight
        )
    row_count, share = samples.shape
    group_count = lax.axis_size("expert")
    gate_count = lax.axis_size("gate")
    expert_count = group_count * gate_count
    capacity = 4 * row_count // expert_count
    partial = jnp.dot(samples, gate_weight, preferred_element_type=jnp.float32)
    logits = jnp.sum(lax.all_gather(partial, "gate"), axis=0)
    first, second, member, before = routing(expert_ids, expert_count)
    place = jnp.where(member, before, -1).T
    ranks = jnp.arange(capacity, dtype=jnp.int32)
    send = (place[:, None, :] == ranks[None, :, None]).astype(jnp.bfloat16)
    outgoing = jnp.dot(
        send.reshape(expert_count * capacity, row_count), samples, preferred_element_type=jnp.float32
    ).astype(jnp.bfloat16)
    incoming = lax.all_to_all(
        outgoing.reshape(expert_count, capacity, share),
        ("expert", "gate"),
        split_axis=0,
        concat_axis=0,
        tiled=True,
    ).reshape(group_count, gate_count, capacity, share)
    hidden = 0.0
    for g in range(gate_count):
        hidden += jnp.dot(
            incoming[:, g].reshape(group_count * capacity, share),
            up_weight[0, g * share : (g + 1) * share],
            preferred_element_type=jnp.float32,
        )
    active = jnp.maximum(hidden, 0.0).astype(jnp.bfloat16)
    expert_out = jnp.dot(active, down_weight[0], preferred_element_type=jnp.float32).astype(
        jnp.bfloat16
    )
    out_share = expert_out.shape[1] // gate_count
    outbound = expert_out.reshape(group_count, capacity, gate_count, out_share)
    outbound = outbound.transpose(0, 2, 1, 3).reshape(expert_count, capacity, out_share)
    returned = lax.all_to_all(
        outbound, ("expert", "gate"), split_axis=0, concat_axis=0, tiled=True
    ).reshape(expert_count * capacity, out_share)
    factor0, factor1 = factors(logits, first, second, pad_mask, expert_count)
    slots = jnp.arange(expert_count * capacity, dtype=jnp.int32)[None, :]
    mixed = 0.0
    for k, (chosen, factor) in enumerate(((first, factor0), (second, factor1))):
        rank = jnp.sum(jnp.where(chosen, before, 0), axis=1, keepdims=True)
        position = expert_ids[:, k : k + 1] * capacity + rank
        pick = (position == slots).astype(jnp.bfloat16)
        mixed += factor * jnp.dot(pick, returned, preferred_element_type=jnp.float32)
    return mixed.astype(jnp.bfloat16)


def solution(mesh):
    placed = (
        P("expert", "gate"),
        P("gate", None),
        P("expert", None),
        P("expert"),
        P(("expert", "gate"), None, None),
        P(("expert", "gate"), None, None),
    )
    return jax.shard_map(
        per_device, mesh=mesh, in_specs=placed, out_specs=P("expert", "gate"), check_vma=False
    )
```
